32 devices in a mesh: section: 4 (over z), fsdp: 4 (over y, core), tp: 2 (over x).
Axes of the slice: x: 2, y: 2, z: 4, core: 2. Of those that a mesh axis runs over, the one named last changes fastest.
Arguments:
- stash: bfloat16 [4, 4, 512, 2304], P('section', None, 'fsdp'), may hold values from -6 to 6
- grad_now: bfloat16 [4, 512, 2304], P('section', 'fsdp'), may hold values from -6 to 6
- grad_top: bfloat16 [2, 512, 2304], P(None, 'fsdp'), may hold values from -6 to 6
- order: int32 [4, 4], P('section'), may hold values from 0 to 3, each once within a row
- gain: float32 [4, 2304], P('section'), may hold values from 0.5 to 1.5
- weight: bfloat16 [4, 2304, 2048], P('section', 'fsdp', 'tp'), may hold values from -0.125 to 0.125
Outputs:
- grad_held: bfloat16 [4, 512, 2304], P('section', 'fsdp')
- weight_grad: float32 [4, 2304, 2048], P('section', 'fsdp', 'tp')
The draws below stay inside these ranges and needn't reach their ends.
Inputs may be any that keep to these rules, and one draw needn't show every extreme that they name: Each row of order names every kept micro-batch once.
All inputs are finite; a program needn't handle non-finite values.
Results may differ from the reference program's by a relative error of at most 0.013.
Values may be sent and summed in bfloat16 or wider, within the bound.
A program may use at most 64 MiB of HBM per device.

```python
import jax
import jax.numpy as jnp
from jax import lax

D = 2304
INNER = 2048
MB = 4
TICKS = 2
SECTIONS = 4
TOKENS = 512
N_TP = 2


def level_of(key, extent, pieces, least, largest):
    def one(axis_at, blocks):
        heights = jax.random.uniform(jax.random.fold_in(jax.random.fold_in(key, 6), axis_at), (blocks,), jnp.float32, least / len(pieces), largest / len(pieces))
        return jnp.repeat(jnp.exp(heights), extent[axis_at] // blocks).reshape((-1,) + (1,) * (len(extent) - axis_at - 1))

    level = one(*pieces[0])
    for cut in pieces[1:]:
        level = level * one(*cut)
    return level


def scatter_about(key, extent, spread, limit, cuts=(), kind=jnp.bfloat16):
    loudness = level_of(key, extent, cuts, -0.22, 0.18) if cuts else 1.0
    drawn = jax.random.normal(key, extent, jnp.float32) * spread * loudness
    return jnp.minimum(jnp.maximum(drawn, -limit), limit).astype(kind)


def setup_inputs(seed: int = 0) -> dict:
    seeds = jax.random.split(jax.random.key(seed), 7)
    stash = scatter_about(seeds[0], (SECTIONS, MB, TOKENS, D), 1.0, 6.0, ((0, 4), (2, 4)))
    grad_now = scatter_about(seeds[1], (SECTIONS, TOKENS, D), 1.0, 6.0, ((0, 4), (1, 4)))
    grad_top = scatter_about(seeds[2], (TICKS, TOKENS, D), 1.0, 6.0, ((1, 4),))
    order = jax.vmap(lambda own: jax.random.permutation(own, MB))(jax.random.split(seeds[3], SECTIONS)).reshape((SECTIONS, MB)).astype(jnp.int32)
    gain = jnp.clip(1.0 + 0.1 * jax.random.normal(seeds[4], (SECTIONS, D), jnp.float32), 0.5, 1.5)
    weight = scatter_about(seeds[5], (SECTIONS, D, INNER), D ** -0.5, 0.125, ((0, 4), (1, 4), (2, 2)))
    return dict(stash=stash, grad_now=grad_now, grad_top=grad_top, order=order, gain=gain, weight=weight)


norm_eps = 1e-06

def gelu_tanh(values):
    return jax.nn.gelu(values, approximate=True)

def section_tick(section_in, grad_in, section_gain, section_weight):
    values = section_in.astype(jnp.float32)
    inv_rms = lax.rsqrt(lax.optimization_barrier(jnp.mean(values * values, axis=-1, keepdims=True)) + norm_eps)
    scaled = values * inv_rms
    normed = (scaled * section_gain).astype(jnp.bfloat16)
    hidden = jnp.dot(normed, section_weight, preferred_element_type=jnp.float32)
    backed = jnp.dot(grad_in, section_weight, preferred_element_type=jnp.float32)
    activated, pullback = jax.vjp(gelu_tanh, hidden)
    grad_pre = pullback(backed)[0].astype(jnp.bfloat16)
    activated = activated.astype(jnp.bfloat16)
    group = section_weight.shape[1] // N_TP
    total = jnp.zeros(values.shape, jnp.float32)
    for member in range(N_TP):
        left = grad_pre[:, member * group:(member + 1) * group]
        right = section_weight[:, member * group:(member + 1) * group]
        partial_dh = lax.dot_general(left, right, (((1,), (1,)), ((), ())), preferred_element_type=jnp.float32)
        rounded = lax.optimization_barrier(partial_dh.astype(jnp.bfloat16))
        total = total + rounded.astype(jnp.float32)
    gained = section_gain * total
    inner_mean = lax.optimization_barrier(jnp.mean(gained * scaled, axis=-1, keepdims=True))
    grad_out = (grad_in.astype(jnp.float32) + inv_rms * (gained - scaled * inner_mean)).astype(jnp.bfloat16)
    return (grad_out, normed, grad_pre, activated)

def reference(stash, grad_now, grad_top, order, gain, weight):
    held = grad_now
    lhs_parts = []
    rhs_parts = []
    for tick_id in range(TICKS):

        def per_section(items):
            section_stash, section_order, grad_in, section_gain, section_weight = items
            slot_id = section_order[tick_id].astype(jnp.int32)
            section_in = lax.dynamic_index_in_dim(section_stash, slot_id, 0, keepdims=False)
            return section_tick(section_in, grad_in, section_gain, section_weight)
        grad_out, normed, grad_pre, activated = lax.map(per_section, (stash, order, held, gain, weight))
        lhs_parts.append(normed)
        lhs_parts.append(held)
        rhs_parts.append(grad_pre)
        rhs_parts.append(activated)
        held = jnp.concatenate([grad_out[1:], grad_top[tick_id][None]], axis=0)
    lhs_all = jnp.concatenate(lhs_parts, axis=1)
    rhs_all = jnp.concatenate(rhs_parts, axis=1)

    def section_grad(items):
        left, right = items
        return lax.dot_general(left, right, (((0,), (0,)), ((), ())), preferred_element_type=jnp.float32)
    weight_grad = lax.map(section_grad, (lhs_all, rhs_all))
    return (held, weight_grad)
```

```python
import functools
import math

import jax
import jax.numpy as jnp
from jax import lax
from jax.experimental import pallas as pl
from jax.experimental.pallas import tpu as pltpu
from jax.sharding import PartitionSpec as P

norm_eps = 1e-06
MESH = pl.DeviceIdType.MESH
f32 = jnp.float32
bf16 = jnp.bfloat16
LAG = 3


def gelu_parts(u):
    k = 0.7978845608028654
    c = 0.044715
    u2 = u * u
    t = jnp.tanh(k * u * (1.0 + c * u2))
    half = 0.5 * (1.0 + t)
    act = u * half
    slope = half + 0.5 * u * (1.0 - t * t) * (k * (1.0 + 3.0 * c * u2))
    return act, slope


def pick(extent, options):
    for o in options:
        if extent % o == 0:
            return o
    return extent


def w_cuts(wl):
    if wl % 64 or wl <= 128:
        return (0, wl)
    deep = wl // 128 * 128
    cuts = list(range(0, deep, 256)) + [deep]
    return tuple(cuts) if deep == wl else tuple(cuts) + (wl,)


def row_step(wl):
    return math.gcd(wl, 64)


def kernel(
    S, FS, TP, T, order_ref, gain_ref, stash_ref, gnow_ref, gtop_ref, w_ref,
    held_ref, acc, lta, rhs,
    wfull, stash, act, xt, inv, dyn, lt, prod, slope, own_e, peer_e, dxs, zin, peer_f,
    lsem, topsem, ownsem, w_s, w_r, l_s, l_r, r_s, r_r, e_s, e_r, z_s, z_r, x_s, x_r, f_s, f_r,
):
    s = lax.axis_index("section")
    f = lax.axis_index("fsdp")
    p = lax.axis_index("tp")
    NC = FS // 2
    yc = f // 2
    core = f % 2
    sib = 2 * yc + (1 - core)
    n, D = act.shape[0] // (T + 1), act.shape[1]
    wl, N = w_ref.shape[1], w_ref.shape[2]
    cuts = w_cuts(wl)
    WCH = len(cuts) - 1
    wq = wl // TP
    CW = D // e_s.shape[-1]
    CH = D // CW
    nw = pick(N, (256, 128))
    tiles = N // nw
    here = CH * s // S
    there = CH * (s + 1) // S

    loads = [
        pltpu.make_async_copy(w_ref.at[0], wfull.at[pl.ds(f * wl, wl), :], lsem.at[0]),
        pltpu.make_async_copy(stash_ref.at[0], stash, lsem.at[1]),
        pltpu.make_async_copy(gnow_ref.at[0], act.at[pl.ds(T * n, n), :], lsem.at[2]),
    ]
    for c in loads:
        c.start()

    bar = pltpu.get_barrier_semaphore()
    for r in range(1, FS):
        pl.semaphore_signal(bar, inc=1, device_id={"fsdp": (f + r) % FS}, device_id_type=MESH)
    for r in range(1, TP):
        pl.semaphore_signal(bar, inc=1, device_id={"tp": (p + r) % TP}, device_id_type=MESH)

    @pl.when(s > 0)
    def _():
        pl.semaphore_signal(bar, inc=1, device_id={"section": s - 1}, device_id_type=MESH)

    @pl.when(s < S - 1)
    def _():
        pl.semaphore_signal(bar, inc=1, device_id={"section": s + 1}, device_id_type=MESH)

    pl.semaphore_wait(bar, FS - 1 + TP - 1 + jnp.minimum(s, 1) + jnp.minimum(S - 1 - s, 1))

    def rcopy(src, dst, ss, rs, dev):
        return pltpu.make_async_remote_copy(
            src_ref=src, dst_ref=dst, send_sem=ss, recv_sem=rs, device_id=dev, device_id_type=MESH
        )

    def w_copy(k, j):
        lo, hi = cuts[j], cuts[j + 1]
        at = pl.multiple_of(lo + core * (wl - hi - lo), row_step(wl))
        if k < NC:
            rows = pl.ds(pl.multiple_of(f * wl + at, row_step(wl)), hi - lo)
            src = w_ref.at[0, pl.ds(at, hi - lo), :]
            to = sib if k == 0 else 2 * ((yc + k) % NC) + core
        else:
            o = k - NC + 1
            rows = pl.ds(pl.multiple_of((2 * ((yc - o + NC) % NC) + core) * wl + at, row_step(wl)), hi - lo)
            src = wfull.at[rows, :]
            to = sib
        return rcopy(src, wfull.at[rows, :], w_s.at[k, j], w_r.at[k, j], {"fsdp": to})

    for k in list(range(1, NC)) + [0]:
        for j in range(WCH):
            w_copy(k, j).start()

    def is_split(part):
        return TP > 1

    def l_copy(part, k):
        cols = pl.ds(pl.multiple_of(f * n, n), n)
        if k == 0:
            to = sib
        else:
            o, cc = (k + 1) // 2, (k - 1) % 2
            to = 2 * ((yc + o) % NC) + (core + cc) % 2
        if k > 0 and is_split(part):
            src = lt.at[part, pl.ds(to * wl + p * wq, wq), :]
            dst = lta.at[part, pl.ds(p * wq, wq), cols]
        else:
            src = lt.at[part, pl.ds(to * wl, wl), :]
            dst = lta.at[part, :, cols]
        return rcopy(src, dst, l_s.at[part, k], l_r.at[part, k], {"fsdp": to})

    def x_copy(part, k, q):
        o, cc = (k + 1) // 2, (k - 1) % 2
        src_f = 2 * ((yc - o + NC) % NC) + (core + cc) % 2
        blk = lta.at[part, pl.ds(p * wq, wq), pl.ds(pl.multiple_of(src_f * n, n), n)]
        return rcopy(blk, blk, x_s.at[part, k - 1, q - 1], x_r.at[part, k - 1, q - 1], {"tp": (p + q) % TP})

    passed = set()

    def l_pass(part):
        if part in passed or not is_split(part):
            return
        passed.add(part)
        for k in range(1, FS - 1):
            l_copy(part, k).wait_recv()
            for q in range(1, TP):
                x_copy(part, k, q).start()

    def l_own(part):
        return pltpu.make_async_copy(
            lt.at[part, pl.ds(f * wl, wl), :], lta.at[part, :, pl.ds(pl.multiple_of(f * n, n), n)],
            ownsem.at[part],
        )

    def l_send(part):
        for k in list(range(1, FS - 1)) + [0]:
            l_copy(part, k).start()
        l_own(part).start()

    def r_copy(part, k):
        if k < NC:
            at = f
            to = sib if k == 0 else 2 * ((yc + k) % NC) + core
        else:
            o = k - NC + 1
            at = 2 * ((yc - o + NC) % NC) + core
            to = sib
        blk = rhs.at[part, pl.ds(pl.multiple_of(at * n, n), n), :]
        return rcopy(blk, blk, r_s.at[part, k], r_r.at[part, k], {"fsdp": to})

    def r_send(part):
        for k in list(range(1, NC)) + [0]:
            r_copy(part, k).start()

    tw = pick(D, (256, 128))

    def transpose_rows(part, ref, first):
        @pl.loop(0, D // tw)
        def _(i):
            cols = pl.ds(pl.multiple_of(i * tw, tw), tw)
            lt[part, cols, :] = ref[pl.ds(first, n), cols].astype(f32).T.astype(bf16)

    loads[1].wait()
    rb = pick(n, (32, 16))
    for t in range(T):
        slot = order_ref[0, t]

        @pl.loop(0, n // rb)
        def _(i):
            rows = pl.ds(pl.multiple_of(i * rb, rb), rb)
            raw = stash[slot, rows, :]
            v = raw.astype(f32)
            iv = lax.rsqrt(jnp.mean(v * v, axis=-1, keepdims=True) + norm_eps)
            xt[t, rows, :] = raw
            inv[t, rows, :] = jnp.broadcast_to(iv, (rb, 128))
            act[pl.ds(pl.multiple_of(t * n + i * rb, rb), rb), :] = ((v * iv) * gain_ref[0:1, :]).astype(bf16)

        transpose_rows(2 * t, act, t * n)
        if t == 0:
            l_send(0)
            loads[2].wait()
            transpose_rows(1, act, T * n)
            l_send(1)
        else:
            l_send(2 * t)

    @pl.when(s == S - 1)
    def _():
        for t in range(T):
            pltpu.make_async_copy(gtop_ref.at[t], zin.at[t], topsem.at[t]).start()

    half = 2 * wl

    def part_product(chip, spans, first):
        @pl.loop(0, tiles)
        def _(i):
            cols = pl.ds(pl.multiple_of(i * nw, nw), nw)
            d = None
            for lo, hi in spans:
                ks = pl.ds(pl.multiple_of(chip * half + lo, math.gcd(half, lo)), hi - lo)
                one = jnp.dot(act[:, ks], wfull[ks, cols], preferred_element_type=f32)
                d = one if d is None else d + one
            if first:
                prod[:, cols] = d
            else:
                prod[:, cols] += d

    loads[0].wait()
    for j in range(WCH):
        w_copy(0, j).wait_recv()
    part_product(yc, [(0, half)], True)
    for o in range(1, NC):
        for j in range(WCH):
            w_copy(o, j).wait_recv()
            w_copy(NC - 1 + o, j).start()
            w_copy(NC - 1 + o, j).wait_recv()
            lo, hi = cuts[j], cuts[j + 1]
            spans = [(lo, half - lo)] if hi == wl else [(lo, hi), (half - hi, half - lo)]
            part_product((yc - o + NC) % NC, spans, False)

    mine = pl.multiple_of(f * n, n)

    def gelu_rows(t, with_grad):
        @pl.loop(0, n // rb)
        def _(i):
            rows = pl.ds(pl.multiple_of(t * n + i * rb, rb), rb)
            home = pl.ds(pl.multiple_of(mine + i * rb, rb), rb)
            a, sl = gelu_parts(prod[rows, :])
            rhs[2 * t + 1, home, :] = a.astype(bf16)
            if with_grad:
                g = prod[pl.ds(pl.multiple_of(T * n + i * rb, rb), rb), :]
                rhs[2 * t, home, :] = (sl * g).astype(bf16)
            else:
                slope[t, pl.ds(pl.multiple_of(i * rb, rb), rb), :] = sl

    def e_copy(t, r, c):
        cols = pl.ds(pl.multiple_of(c * CW, CW), CW)
        return rcopy(
            own_e.at[t, :, cols], peer_e.at[t, r - 1, :, cols],
            e_s.at[t, r - 1, c], e_r.at[t, r - 1, c], {"tp": (p + r) % TP},
        )

    def f_copy(t, r, c):
        cols = pl.ds(pl.multiple_of(c * CW, CW), CW)
        return rcopy(
            zin.at[t, :, cols], peer_f.at[t, r - 1, :, cols],
            f_s.at[t, r - 1, c], f_r.at[t, r - 1, c], {"tp": (p + r) % TP},
        )

    def z_copy(t, c, src):
        cols = pl.ds(pl.multiple_of(c * CW, CW), CW)
        to = jnp.maximum(s - 1, 0)
        return rcopy(
            src.at[t, :, cols], zin.at[t, :, cols], z_s.at[t, c], z_r.at[t, c], {"section": to}
        )

    def held_dy(t, cols):
        return (act[pl.ds(T * n, n), cols] if t == 0 else dyn[t - 1, :, cols]).astype(f32)

    def spread(t):
        du = rhs[2 * t, pl.ds(mine, n), :]
        u = prod[pl.ds(t * n, n), :]
        m = jnp.sum(du.astype(f32) * u, axis=-1, keepdims=True) / D
        iv = inv[t, :, 0:1]
        q_scale = iv * iv * m

        @pl.loop(0, CH)
        def _(i):
            c = CH - 1 - i
            cols = pl.ds(pl.multiple_of(c * CW, CW), CW)
            dh = lax.dot_general(
                rhs[2 * t, pl.ds(mine, n), :], wfull[cols, :], (((1,), (1,)), ((), ())),
                preferred_element_type=f32,
            )
            e = iv * (gain_ref[0:1, cols] * dh) - xt[t, :, cols].astype(f32) * q_scale
            own_e[t, :, cols] = jnp.where((c >= here) & (p == 0), e + held_dy(t, cols), e).astype(bf16)

            @pl.when(c >= here)
            def _():
                z_copy(t, c, own_e).start()

            @pl.when(c < here)
            def _():
                for r in range(1, TP):
                    e_copy(t, r, c).start()

    def combine(t, c):
        cols = pl.ds(pl.multiple_of(c * CW, CW), CW)
        for r in range(1, TP):
            e_copy(t, r, c).wait_recv()
        total = own_e[t, :, cols].astype(f32)
        for r in range(1, TP):
            total = total + peer_e[t, r - 1, :, cols].astype(f32)
        dxs[t, :, cols] = (held_dy(t, cols) + total).astype(bf16)
        z_copy(t, c, dxs).start()

    def forward(t, c):
        z_copy(t, c, dxs).wait_recv()
        for r in range(1, TP):
            f_copy(t, r, c).start()

    def put(t, cols, value):
        if t == T - 1:
            held_ref[0, :, cols] = value
        else:
            dyn[t, :, cols] = value

    def arrive(t, c):
        cols = pl.ds(pl.multiple_of(c * CW, CW), CW)

        @pl.when((c < there) & (s < S - 1))
        def _():
            z_copy(t, c, dxs).wait_recv()

        @pl.when(c < there)
        def _():
            put(t, cols, zin[t, :, cols])

        @pl.when(c >= there)
        def _():
            total = zin[t, :, cols].astype(f32)
            for r in range(1, TP):
                f_copy(t, r, c).wait_recv()
                total = total + peer_f[t, r - 1, :, cols].astype(f32)
            put(t, cols, total.astype(bf16))

        return cols

    def relay_loop(t, consume, service):
        @pl.loop(0, CH + LAG)
        def _(i):
            @pl.when(i < CH - there)
            def _():
                forward(t, CH - 1 - i)

            @pl.when(i < here)
            def _():
                combine(t, here - 1 - i)

            service(i)

            @pl.when(i >= LAG)
            def _():
                j = i - LAG
                consume(j, CH - 1 - j)

    def at_step(i, step, fn):
        @pl.when(i == step)
        def _():
            fn()

    relayed = set()

    def r_relay(part):
        if part in relayed:
            return
        relayed.add(part)
        for o in range(1, NC):
            r_copy(part, o).wait_recv()
            r_copy(part, NC - 1 + o).start()

    parts = []
    for t in range(T):
        parts += [2 * t, 2 * t + 1] if t == 0 else [2 * t + 1, 2 * t]

    def own_wait(part):
        l_own(part).wait()
        l_copy(part, 0).wait_recv()
        for k in range(1, FS - 1):
            if is_split(part):
                for q in range(1, TP):
                    x_copy(part, k, q).wait_recv()
            else:
                l_copy(part, k).wait_recv()
        r_copy(part, 0).wait_recv()
        for o in range(1, NC):
            r_copy(part, NC - 1 + o).wait_recv()

    def own_tile(at, i):
        part = parts[at]
        cols = pl.ds(pl.multiple_of(i * nw, nw), nw)
        d = jnp.dot(lta[part], rhs[part, :, cols], preferred_element_type=f32)
        if at > 0:
            d = acc[:, cols] + d
        acc[:, cols] = d

    for t in range(T):
        last = t == T - 1
        if t == 0:
            gelu_rows(0, True)
            r_send(0)
            r_send(1)
        else:
            r_send(2 * t)

        @pl.when(s > 0)
        def _():
            spread(t)

        if t == 0:
            for later in range(1, T):
                gelu_rows(later, False)
                r_send(2 * later + 1)

        @pl.when(s == S - 1)
        def _():
            pltpu.make_async_copy(gtop_ref.at[t], zin.at[t], topsem.at[t]).wait()

        if not last:
            gr = pl.ds(T * n, n)

            def consume(j, c):
                cols = arrive(t, c)
                d = dyn[t, :, cols]
                lt[2 * t + 3, cols, :] = d.astype(f32).T.astype(bf16)
                g = jnp.dot(d, wfull[cols, :], preferred_element_type=f32)

                @pl.when(j == 0)
                def _():
                    prod[gr, :] = g

                @pl.when(j > 0)
                def _():
                    prod[gr, :] += g

            def service(i):
                if t == 0:
                    at_step(i, jnp.where(s == 0, 0, CH - 2), lambda: l_pass(0))
                    at_step(i, jnp.where(s == 0, CH + LAG - 1, CH), lambda: l_pass(1))
                    at_step(i, CH + LAG - 1, lambda: r_relay(0))

            relay_loop(t, consume, service)
            l_send(2 * t + 3)

            @pl.loop(0, n // rb)
            def _(i):
                rows = pl.ds(pl.multiple_of(i * rb, rb), rb)
                g = prod[pl.ds(pl.multiple_of(T * n + i * rb, rb), rb), :]
                here_rows = pl.ds(pl.multiple_of(mine + i * rb, rb), rb)
                rhs[2 * t + 2, here_rows, :] = (slope[t + 1, rows, :] * g).astype(bf16)
        else:
            late = len(parts) - 1
            fill = max(late - 1, 0)

            def consume(j, c):
                arrive(t, c)

            def begin(at):
                part = parts[at]
                l_pass(part)
                r_relay(part)
                own_wait(part)

            def service(i):
                if fill > 1:
                    at_step(i, 0, lambda: r_relay(parts[1]))
                    at_step(i, jnp.where(s == 0, 0, CH - 2), lambda: l_pass(parts[late]))
                    at_step(i, CH - 1, lambda: l_pass(parts[fill]))
                    at_step(i, CH - 1, lambda: r_relay(parts[fill]))
                for k in range(fill):
                    @pl.when((i >= k * tiles) & (i < (k + 1) * tiles))
                    def _():
                        @pl.when(i == k * tiles)
                        def _():
                            begin(k)

                        own_tile(k, i - k * tiles)

            relay_loop(t, consume, service)
            steps = CH + LAG
            for k in range(fill):
                if k * tiles >= steps:
                    begin(k)
                for i in range(max(steps - k * tiles, 0), tiles):
                    own_tile(k, i)
            if late > 0:
                begin(fill)

                @pl.loop(0, tiles)
                def _(i):
                    own_tile(fill, i)

            begin(late)

    for j in range(WCH):
        for k in range(2 * NC - 1):
            w_copy(k, j).wait_send()
    for part in range(2 * T):
        for k in range(FS - 1):
            l_copy(part, k).wait_send()
        if is_split(part):
            for k in range(1, FS - 1):
                for q in range(1, TP):
                    x_copy(part, k, q).wait_send()
        for k in range(2 * NC - 1):
            r_copy(part, k).wait_send()

    for t in range(T):
        @pl.loop(0, CH)
        def _(c):
            @pl.when(c < here)
            def _():
                for r in range(1, TP):
                    e_copy(t, r, c).wait_send()

            @pl.when(c >= there)
            def _():
                for r in range(1, TP):
                    f_copy(t, r, c).wait_send()

            @pl.when(s > 0)
            def _():
                z_copy(t, c, dxs).wait_send()


def finish(part, held_in, acc, lta, rhs, held_ref, wg_ref, grad, sem):
    N = acc.shape[1]
    nw = pick(N, (256, 128))
    tiles = N // nw
    held = pltpu.make_async_copy(held_in, held_ref, sem.at[tiles])
    held.start()

    def tile_copy(i):
        cols = pl.ds(i * nw, nw)
        return pltpu.make_async_copy(grad.at[:, cols], wg_ref.at[0, :, cols], sem.at[i])

    for i in range(tiles):
        cols = pl.ds(i * nw, nw)
        grad[:, cols] = acc[:, cols] + jnp.dot(lta[part], rhs[part, :, cols], preferred_element_type=f32)
        tile_copy(i).start()
    for i in range(tiles):
        tile_copy(i).wait()
    held.wait()


def solution(mesh):
    S, FS, TP = mesh.shape["section"], mesh.shape["fsdp"], mesh.shape["tp"]

    def per_device(stash, grad_now, grad_top, order, gain, weight):
        MB, n, D = stash.shape[1:]
        T = grad_top.shape[0]
        wl, N = weight.shape[1:]
        NC = FS // 2
        CH = D // pick(D, (256, 128))
        WCH = len(w_cuts(wl)) - 1
        K = 2 * NC - 1
        DMA = pltpu.SemaphoreType.DMA
        V = pltpu.VMEM
        any_ = pl.BlockSpec(memory_space=pl.ANY)
        vmem = pl.BlockSpec(memory_space=V)
        peers = max(TP - 1, 1)
        outs = pl.pallas_call(
            functools.partial(kernel, S, FS, TP, T),
            out_shape=(
                V((1, n, D), bf16),
                V((wl, N), f32),
                V((2 * T, wl, FS * n), bf16),
                V((2 * T, FS * n, N), bf16),
            ),
            in_specs=[
                pl.BlockSpec(memory_space=pltpu.SMEM),
                pl.BlockSpec(memory_space=pltpu.VMEM),
                any_, any_, any_, any_,
            ],
            out_specs=(vmem,) * 4,
            scratch_shapes=[
                V((FS * wl, N), bf16),
                V((MB, n, D), bf16),
                V(((T + 1) * n, D), bf16),
                V((T, n, D), bf16),
                V((T, n, 128), f32),
                V((T, n, D), bf16),
                V((2 * T, D, n), bf16),
                V(((T + 1) * n, N), f32),
                V((T, n, N), f32),
                V((T, n, D), bf16),
                V((T, peers, n, D), bf16),
                V((T, n, D), bf16),
                V((T, n, D), bf16),
                V((T, peers, n, D), bf16),
                DMA((3,)), DMA((T,)), DMA((2 * T,)),
                DMA((K, WCH)), DMA((K, WCH)),
                DMA((2 * T, FS - 1)), DMA((2 * T, FS - 1)),
                DMA((2 * T, K)), DMA((2 * T, K)),
                DMA((T, peers, CH)), DMA((T, peers, CH)),
                DMA((T, CH)), DMA((T, CH)),
                DMA((2 * T, max(FS - 2, 1), peers)), DMA((2 * T, max(FS - 2, 1), peers)),
                DMA((T, peers, CH)), DMA((T, peers, CH)),
            ],
            compiler_params=pltpu.CompilerParams(
                collective_id=0, has_side_effects=True, vmem_limit_bytes=44 * 1024 * 1024
            ),
        )(*[pltpu.with_memory_space_constraint(o, pltpu.HBM) for o in (order, gain, stash, grad_now, grad_top, weight)])
        return pl.pallas_call(
            functools.partial(finish, 2 * T - 2 if T > 1 else 1),
            out_shape=(
                jax.ShapeDtypeStruct((1, n, D), bf16),
                jax.ShapeDtypeStruct((1, wl, N), f32),
            ),
            in_specs=[vmem] * 4,
            out_specs=(any_, any_),
            scratch_shapes=[V((wl, N), f32), DMA((N // pick(N, (256, 128)) + 1,))],
            compiler_params=pltpu.CompilerParams(vmem_limit_bytes=8 * 1024 * 1024),
        )(*[pltpu.with_memory_space_constraint(o, V) for o in outs])

    return jax.shard_map(
        per_device,
        mesh=mesh,
        in_specs=(
            P("section", None, "fsdp", None),
            P("section", "fsdp", None),
            P(None, "fsdp", None),
            P("section", None),
            P("section", None),
            P("section", "fsdp", "tp"),
        ),
        out_specs=(P("section", "fsdp", None), P("section", "fsdp", "tp")),
        check_vma=False,
    )
```

```python
import functools
import math

import jax
import jax.numpy as jnp
from jax import lax
from jax.experimental import pallas as pl
from jax.experimental.pallas import tpu as pltpu
from jax.sharding import PartitionSpec as P

norm_eps = 1e-06
MESH = pl.DeviceIdType.MESH
f32 = jnp.float32
bf16 = jnp.bfloat16
LAG = 3


def gelu_parts(u):
    k = 0.7978845608028654
    c = 0.044715
    u2 = u * u
    t = jnp.tanh(k * u * (1.0 + c * u2))
    half = 0.5 * (1.0 + t)
    act = u * half
    slope = half + 0.5 * u * (1.0 - t * t) * (k * (1.0 + 3.0 * c * u2))
    return act, slope


def pick(extent, options):
    for o in options:
        if extent % o == 0:
            return o
    return extent


def w_cuts(wl):
    if wl % 64 or wl <= 128:
        return (0, wl)
    deep = wl // 128 * 128
    cuts = list(range(0, deep, 256)) + [deep]
    return tuple(cuts) if deep == wl else tuple(cuts) + (wl,)


def row_step(wl):
    return math.gcd(wl, 64)


def kernel(
    S, FS, TP, T, order_ref, gain_ref, stash_ref, gnow_ref, gtop_ref, w_ref,
    held_ref, acc, lta, rhs,
    wfull, stash, act, xt, inv, dyn, lt, prod, slope, own_e, peer_e, dxs, zin,
    lsem, topsem, w_s, w_r, l_s, l_r, r_s, r_r, e_s, e_r, z_s, z_r, x_s, x_r,
):
    s = lax.axis_index("section")
    f = lax.axis_index("fsdp")
    p = lax.axis_index("tp")
    NC = FS // 2
    SPLIT = (0, 1, 2)
    yc = f // 2
    core = f % 2
    sib = 2 * yc + (1 - core)
    n, D = act.shape[0] // (T + 1), act.shape[1]
    wl, N = w_ref.shape[1], w_ref.shape[2]
    cuts = w_cuts(wl)
    WCH = len(cuts) - 1
    wq = wl // TP
    CW = D // e_s.shape[-1]
    CH = D // CW
    nw = pick(N, (256, 128))
    tiles = N // nw
    here = CH * s // S
    there = CH * (s + 1) // S
    free = jnp.maximum(here, CH - there)

    loads = [
        pltpu.make_async_copy(w_ref.at[0], wfull.at[pl.ds(f * wl, wl), :], lsem.at[0]),
        pltpu.make_async_copy(stash_ref.at[0], stash, lsem.at[1]),
        pltpu.make_async_copy(gnow_ref.at[0], act.at[pl.ds(T * n, n), :], lsem.at[2]),
    ]
    for c in loads:
        c.start()

    bar = pltpu.get_barrier_semaphore()
    for r in range(1, FS):
        pl.semaphore_signal(bar, inc=1, device_id={"fsdp": (f + r) % FS}, device_id_type=MESH)
    for r in range(1, TP):
        pl.semaphore_signal(bar, inc=1, device_id={"tp": (p + r) % TP}, device_id_type=MESH)

    @pl.when(s > 0)
    def _():
        pl.semaphore_signal(bar, inc=1, device_id={"section": s - 1}, device_id_type=MESH)

    @pl.when(s < S - 1)
    def _():
        pl.semaphore_signal(bar, inc=1, device_id={"section": s + 1}, device_id_type=MESH)

    pl.semaphore_wait(bar, FS - 1 + TP - 1 + jnp.minimum(s, 1) + jnp.minimum(S - 1 - s, 1))

    def rcopy(src, dst, ss, rs, dev):
        return pltpu.make_async_remote_copy(
            src_ref=src, dst_ref=dst, send_sem=ss, recv_sem=rs, device_id=dev, device_id_type=MESH
        )

    def w_copy(k, j):
        lo, hi = cuts[j], cuts[j + 1]
        at = pl.multiple_of(lo + core * (wl - hi - lo), row_step(wl))
        if k < NC:
            rows = pl.ds(pl.multiple_of(f * wl + at, row_step(wl)), hi - lo)
            to = 2 * ((yc + k) % NC) + core
        else:
            o = k - NC + 1
            rows = pl.ds(pl.multiple_of((2 * ((yc - o + NC) % NC) + core) * wl + at, row_step(wl)), hi - lo)
            to = sib
        blk = wfull.at[rows, :]
        return rcopy(blk, blk, w_s.at[0], w_r.at[1 + (k - 1) * WCH + j], {"fsdp": to})

    def w_sib():
        blk = wfull.at[pl.ds(pl.multiple_of(f * wl, row_step(wl)), wl), :]
        return rcopy(blk, blk, w_s.at[0], w_r.at[0], {"fsdp": sib})

    loads[0].wait()
    for k in range(1, NC):
        for j in range(WCH):
            w_copy(k, j).start()
    w_sib().start()

    def is_split(part):
        return part in SPLIT and TP > 1

    def l_copy(part, k):
        cols = pl.ds(pl.multiple_of(f * n, n), n)
        if k == 0:
            to = sib
        else:
            o, cc = (k + 1) // 2, (k - 1) % 2
            to = 2 * ((yc + o) % NC) + (core + cc) % 2
        if k > 0 and is_split(part):
            src = lt.at[part, pl.ds(to * wl + p * wq, wq), :]
            dst = lta.at[part, pl.ds(p * wq, wq), cols]
        else:
            src = lt.at[part, pl.ds(to * wl, wl), :]
            dst = lta.at[part, :, cols]
        return rcopy(src, dst, l_s.at[part], l_r.at[part, min(k, 1)], {"fsdp": to})

    def x_copy(part, k, q):
        o, cc = (k + 1) // 2, (k - 1) % 2
        src_f = 2 * ((yc - o + NC) % NC) + (core + cc) % 2
        blk = lta.at[part, pl.ds(p * wq, wq), pl.ds(pl.multiple_of(src_f * n, n), n)]
        return rcopy(blk, blk, x_s.at[part], x_r.at[part], {"tp": (p + q) % TP})

    passed = set()

    def l_pass(part):
        if part in passed or not is_split(part):
            return
        passed.add(part)
        l_far(part).wait_recv()
        for k in range(1, FS - 1):
            for q in range(1, TP):
                x_copy(part, k, q).start()

    def rows_of(part, rows, ss, rs):
        blk = lt.at[part, pl.ds(0, rows), :]
        return rcopy(blk, blk, ss, rs, {"fsdp": sib})

    def l_far(part):
        return rows_of(part, (FS - 2) * (wq if is_split(part) else wl), l_s.at[part], l_r.at[part, 1])

    def l_sent(part):
        return rows_of(part, wl + (FS - 2) * (wq if is_split(part) else wl), l_s.at[part], l_r.at[part, 1])

    def x_all(part):
        return rows_of(part, (FS - 2) * (TP - 1) * wq, x_s.at[part], x_r.at[part])

    def r_rows(part, count, which):
        blk = rhs.at[part, pl.ds(0, count * n), :]
        return rcopy(blk, blk, r_s.at[part], r_r.at[part, which], {"fsdp": sib})

    def l_send(part):
        for k in list(range(1, FS - 1)) + [0]:
            l_copy(part, k).start()
        lta[part, :, pl.ds(pl.multiple_of(f * n, n), n)] = lt[part, pl.ds(pl.multiple_of(f * wl, row_step(wl)), wl), :]

    def r_copy(part, k):
        if k < NC:
            at = f
            to = sib if k == 0 else 2 * ((yc + k) % NC) + core
        else:
            o = k - NC + 1
            at = 2 * ((yc - o + NC) % NC) + core
            to = sib
        blk = rhs.at[part, pl.ds(pl.multiple_of(at * n, n), n), :]
        return rcopy(blk, blk, r_s.at[part], r_r.at[part, k if 0 < k < NC else 0], {"fsdp": to})

    def r_send(part):
        for k in list(range(1, NC)) + [0]:
            r_copy(part, k).start()

    tw = pick(D, (256, 128))

    def transpose_rows(part, ref, first):
        @pl.loop(0, D // tw)
        def _(i):
            cols = pl.ds(pl.multiple_of(i * tw, tw), tw)
            lt[part, cols, :] = ref[pl.ds(first, n), cols].astype(f32).T.astype(bf16)

    loads[1].wait()
    rb = pick(n, (32, 16))
    for t in range(T):
        slot = order_ref[0, t]

        @pl.loop(0, n // rb)
        def _(i):
            rows = pl.ds(pl.multiple_of(i * rb, rb), rb)
            raw = stash[slot, rows, :]
            v = raw.astype(f32)
            iv = lax.rsqrt(jnp.mean(v * v, axis=-1, keepdims=True) + norm_eps)
            xt[t, rows, :] = raw
            inv[t, rows, :] = jnp.broadcast_to(iv, (rb, 128))
            act[pl.ds(pl.multiple_of(t * n + i * rb, rb), rb), :] = ((v * iv) * gain_ref[0:1, :]).astype(bf16)

        transpose_rows(2 * t, act, t * n)
        if t == 0:
            l_send(0)
            loads[2].wait()
            transpose_rows(1, act, T * n)
            l_send(1)
        else:
            l_send(2 * t)

    @pl.when(s == S - 1)
    def _():
        for t in range(T):
            pltpu.make_async_copy(gtop_ref.at[t], zin.at[t], topsem.at[t]).start()

    half = 2 * wl

    def part_product(chip, spans, first):
        @pl.loop(0, tiles)
        def _(i):
            cols = pl.ds(pl.multiple_of(i * nw, nw), nw)
            d = None
            for lo, hi in spans:
                ks = pl.ds(pl.multiple_of(chip * half + lo, math.gcd(half, lo)), hi - lo)
                one = jnp.dot(act[:, ks], wfull[ks, cols], preferred_element_type=f32)
                d = one if d is None else d + one
            if first:
                prod[:, cols] = d
            else:
                prod[:, cols] += d

    w_sib().wait_recv()
    part_product(yc, [(0, half)], True)
    for o in range(1, NC):
        for j in range(WCH):
            w_copy(o, j).wait_recv()
            w_copy(NC - 1 + o, j).start()
            w_copy(NC - 1 + o, j).wait_recv()
            lo, hi = cuts[j], cuts[j + 1]
            spans = [(lo, half - lo)] if hi == wl else [(lo, hi), (half - hi, half - lo)]
            part_product((yc - o + NC) % NC, spans, False)

    mine = pl.multiple_of(f * n, n)

    def gelu_rows(t, with_grad):
        @pl.loop(0, n // rb)
        def _(i):
            rows = pl.ds(pl.multiple_of(t * n + i * rb, rb), rb)
            home = pl.ds(pl.multiple_of(mine + i * rb, rb), rb)
            a, sl = gelu_parts(prod[rows, :])
            rhs[2 * t + 1, home, :] = a.astype(bf16)
            if with_grad:
                g = prod[pl.ds(pl.multiple_of(T * n + i * rb, rb), rb), :]
                rhs[2 * t, home, :] = (sl * g).astype(bf16)
            else:
                slope[t, pl.ds(pl.multiple_of(i * rb, rb), rb), :] = sl

    def e_copy(t, r, c):
        cols = pl.ds(pl.multiple_of(c * CW, CW), CW)
        return rcopy(
            own_e.at[t, :, cols], peer_e.at[t, r - 1, :, cols],
            e_s.at[t, r - 1, c], e_r.at[t, r - 1, c], {"tp": (p + r) % TP},
        )

    def f_copy(t, r, c):
        cols = pl.ds(pl.multiple_of(c * CW, CW), CW)
        return rcopy(
            zin.at[t, :, cols], peer_e.at[t, r - 1, :, cols],
            e_s.at[t, r - 1, c], e_r.at[t, r - 1, c], {"tp": (p + r) % TP},
        )

    def z_copy(t, c, src):
        cols = pl.ds(pl.multiple_of(c * CW, CW), CW)
        to = jnp.maximum(s - 1, 0)
        return rcopy(
            src.at[t, :, cols], zin.at[t, :, cols], z_s.at[t, c], z_r.at[t, c], {"section": to}
        )

    def held_dy(t, cols):
        return (act[pl.ds(T * n, n), cols] if t == 0 else dyn[t - 1, :, cols]).astype(f32)

    def spread(t):
        du = rhs[2 * t, pl.ds(mine, n), :]
        u = prod[pl.ds(t * n, n), :]
        m = jnp.sum(du.astype(f32) * u, axis=-1, keepdims=True) / D
        iv = inv[t, :, 0:1]
        q_scale = iv * iv * m

        @pl.loop(0, CH)
        def _(i):
            both = jnp.minimum(here, CH - here)
            far_turn = jnp.where(i < 2 * both, i % 2 == 0, CH - here > here)
            turn = jnp.where(i < 2 * both, i // 2, i - both)
            c = jnp.where(far_turn, CH - 1 - turn, here - 1 - turn)
            cols = pl.ds(pl.multiple_of(c * CW, CW), CW)
            dh = lax.dot_general(
                rhs[2 * t, pl.ds(mine, n), :], wfull[cols, :], (((1,), (1,)), ((), ())),
                preferred_element_type=f32,
            )
            e = iv * (gain_ref[0:1, cols] * dh) - xt[t, :, cols].astype(f32) * q_scale
            own_e[t, :, cols] = jnp.where((c >= here) & (p == 0), e + held_dy(t, cols), e).astype(bf16)

            @pl.when(c >= here)
            def _():
                z_copy(t, c, own_e).start()

            @pl.when(c < here)
            def _():
                for r in range(1, TP):
                    e_copy(t, r, c).start()

    def combine(t, c):
        cols = pl.ds(pl.multiple_of(c * CW, CW), CW)
        for r in range(1, TP):
            e_copy(t, r, c).wait_recv()
        total = own_e[t, :, cols].astype(f32)
        for r in range(1, TP):
            total = total + peer_e[t, r - 1, :, cols].astype(f32)
        dxs[t, :, cols] = (held_dy(t, cols) + total).astype(bf16)
        z_copy(t, c, dxs).start()

    def forward(t, c):
        z_copy(t, c, dxs).wait_recv()
        for r in range(1, TP):
            f_copy(t, r, c).start()

    def put(t, cols, value):
        if t == T - 1:
            held_ref[0, :, cols] = value
        else:
            dyn[t, :, cols] = value

    def arrive(t, c):
        cols = pl.ds(pl.multiple_of(c * CW, CW), CW)

        @pl.when((c < there) & (s < S - 1))
        def _():
            z_copy(t, c, dxs).wait_recv()

        @pl.when(c < there)
        def _():
            put(t, cols, zin[t, :, cols])

        @pl.when(c >= there)
        def _():
            total = zin[t, :, cols].astype(f32)
            for r in range(1, TP):
                f_copy(t, r, c).wait_recv()
                total = total + peer_e[t, r - 1, :, cols].astype(f32)
            put(t, cols, total.astype(bf16))

        return cols

    def relay_loop(t, consume, service):
        @pl.loop(0, CH + LAG)
        def _(i):
            @pl.when(i < CH - there)
            def _():
                forward(t, CH - 1 - i)

            @pl.when(i < here)
            def _():
                combine(t, here - 1 - i)

            service(i)

            @pl.when(i >= LAG)
            def _():
                j = i - LAG
                consume(j, CH - 1 - j)

    def at_step(i, step, fn):
        @pl.when(i == step)
        def _():
            fn()

    relayed = set()

    def r_relay(part):
        if part in relayed:
            return
        relayed.add(part)
        for o in range(1, NC):
            r_copy(part, o).wait_recv()
            r_copy(part, NC - 1 + o).start()

    parts = []
    for t in range(T):
        parts += [2 * t, 2 * t + 1] if t == 0 else [2 * t + 1, 2 * t]

    def own_wait(part):
        l_copy(part, 0).wait_recv()
        if is_split(part):
            x_all(part).wait_recv()
        elif FS > 2:
            l_far(part).wait_recv()
        r_rows(part, NC, 0).wait_recv()

    def own_tile(at, i):
        part = parts[at]
        cols = pl.ds(pl.multiple_of(i * nw, nw), nw)
        d = jnp.dot(lta[part], rhs[part, :, cols], preferred_element_type=f32)
        if at > 0:
            d = acc[:, cols] + d
        acc[:, cols] = d

    for t in range(T):
        last = t == T - 1
        if t == 0:
            gelu_rows(0, True)
            r_send(0)
            r_send(1)
        else:
            r_send(2 * t)

        @pl.when(s > 0)
        def _():
            spread(t)

        if t == 0:
            for later in range(1, T):
                gelu_rows(later, False)
                r_send(2 * later + 1)

        @pl.when(s == S - 1)
        def _():
            pltpu.make_async_copy(gtop_ref.at[t], zin.at[t], topsem.at[t]).wait()

        if not last:
            gr = pl.ds(T * n, n)

            def consume(j, c):
                cols = arrive(t, c)
                d = dyn[t, :, cols]
                lt[2 * t + 3, cols, :] = d.astype(f32).T.astype(bf16)
                g = jnp.dot(d, wfull[cols, :], preferred_element_type=f32)

                @pl.when(j == 0)
                def _():
                    prod[gr, :] = g

                @pl.when(j > 0)
                def _():
                    prod[gr, :] += g

            def service(i):
                if t == 0:
                    at_step(i, free, lambda: (l_pass(0), l_pass(1)))
                    at_step(i, CH + LAG - 1, lambda: r_relay(0))

            relay_loop(t, consume, service)
            l_send(2 * t + 3)

            @pl.loop(0, n // rb)
            def _(i):
                rows = pl.ds(pl.multiple_of(i * rb, rb), rb)
                g = prod[pl.ds(pl.multiple_of(T * n + i * rb, rb), rb), :]
                here_rows = pl.ds(pl.multiple_of(mine + i * rb, rb), rb)
                rhs[2 * t + 2, here_rows, :] = (slope[t + 1, rows, :] * g).astype(bf16)
        else:
            late = len(parts) - 1
            fill = max(late - 1, 0)

            def consume(j, c):
                arrive(t, c)

            def begin(at):
                part = parts[at]
                l_pass(part)
                r_relay(part)
                own_wait(part)

            def service(i):
                if fill > 1:
                    at_step(i, 0, lambda: r_relay(parts[1]))
                    at_step(i, free, lambda: l_pass(parts[late]))
                    at_step(i, CH - 1, lambda: l_pass(parts[fill]))
                    at_step(i, CH - 1, lambda: r_relay(parts[fill]))
                for k in range(fill):
                    @pl.when((i >= k * tiles) & (i < (k + 1) * tiles))
                    def _():
                        @pl.when(i == k * tiles)
                        def _():
                            begin(k)

                        own_tile(k, i - k * tiles)

            relay_loop(t, consume, service)
            steps = CH + LAG
            for k in range(fill):
                if k * tiles >= steps:
                    begin(k)
                for i in range(max(steps - k * tiles, 0), tiles):
                    own_tile(k, i)
            if late > 0:
                begin(fill)

                @pl.loop(0, tiles)
                def _(i):
                    own_tile(fill, i)

            begin(late)

    w_rows = wfull.at[pl.ds(0, (2 * NC - 1) * wl), :]
    rcopy(w_rows, w_rows, w_s.at[0], w_r.at[0], {"fsdp": sib}).wait_send()
    for part in range(2 * T):
        l_sent(part).wait_send()
        if is_split(part) and FS > 2:
            x_all(part).wait_send()
        r_rows(part, 2 * NC - 1, 0).wait_send()

    for t in range(T):
        @pl.loop(0, CH)
        def _(c):
            @pl.when((c < here) | (c >= there))
            def _():
                for r in range(1, TP):
                    e_copy(t, r, c).wait_send()

            @pl.when(s > 0)
            def _():
                z_copy(t, c, dxs).wait_send()


def finish(part, held_in, acc, lta, rhs, held_ref, wg_ref, grad, sem):
    N = acc.shape[1]
    nw = pick(N, (256, 128))
    tiles = N // nw
    held = pltpu.make_async_copy(held_in, held_ref, sem.at[tiles])
    held.start()

    def tile_copy(i):
        cols = pl.ds(i * nw, nw)
        return pltpu.make_async_copy(grad.at[:, cols], wg_ref.at[0, :, cols], sem.at[i])

    for i in range(tiles):
        cols = pl.ds(i * nw, nw)
        grad[:, cols] = acc[:, cols] + jnp.dot(lta[part], rhs[part, :, cols], preferred_element_type=f32)
        tile_copy(i).start()
    for i in range(tiles):
        tile_copy(i).wait()
    held.wait()


def solution(mesh):
    S, FS, TP = mesh.shape["section"], mesh.shape["fsdp"], mesh.shape["tp"]

    def per_device(stash, grad_now, grad_top, order, gain, weight):
        MB, n, D = stash.shape[1:]
        T = grad_top.shape[0]
        wl, N = weight.shape[1:]
        NC = FS // 2
        CH = D // pick(D, (256, 128))
        WCH = len(w_cuts(wl)) - 1
        K = 2 * NC - 1
        DMA = pltpu.SemaphoreType.DMA
        V = pltpu.VMEM
        any_ = pl.BlockSpec(memory_space=pl.ANY)
        vmem = pl.BlockSpec(memory_space=V)
        peers = max(TP - 1, 1)
        outs = pl.pallas_call(
            functools.partial(kernel, S, FS, TP, T),
            out_shape=(
                V((1, n, D), bf16),
                V((wl, N), f32),
                V((2 * T, wl, FS * n), bf16),
                V((2 * T, FS * n, N), bf16),
            ),
            in_specs=[
                pl.BlockSpec(memory_space=pltpu.SMEM),
                pl.BlockSpec(memory_space=pltpu.VMEM),
                any_, any_, any_, any_,
            ],
            out_specs=(vmem,) * 4,
            scratch_shapes=[
                V((FS * wl, N), bf16),
                V((MB, n, D), bf16),
                V(((T + 1) * n, D), bf16),
                V((T, n, D), bf16),
                V((T, n, 128), f32),
                V((T, n, D), bf16),
                V((2 * T, D, n), bf16),
                V(((T + 1) * n, N), f32),
                V((T, n, N), f32),
                V((T, n, D), bf16),
                V((T, peers, n, D), bf16),
                V((T, n, D), bf16),
                V((T, n, D), bf16),
                DMA((3,)), DMA((T,)),
                DMA((1,)), DMA((1 + (K - 1) * WCH,)),
                DMA((2 * T,)), DMA((2 * T, 2)),
                DMA((2 * T,)), DMA((2 * T, NC)),
                DMA((T, peers, CH)), DMA((T, peers, CH)),
                DMA((T, CH)), DMA((T, CH)),
                DMA((2 * T,)), DMA((2 * T,)),
            ],
            compiler_params=pltpu.CompilerParams(
                collective_id=0, has_side_effects=True, vmem_limit_bytes=44 * 1024 * 1024
            ),
        )(*[pltpu.with_memory_space_constraint(o, pltpu.HBM) for o in (order, gain, stash, grad_now, grad_top, weight)])
        return pl.pallas_call(
            functools.partial(finish, 2 * T - 2 if T > 1 else 1),
            out_shape=(
                jax.ShapeDtypeStruct((1, n, D), bf16),
                jax.ShapeDtypeStruct((1, wl, N), f32),
            ),
            in_specs=[vmem] * 4,
            out_specs=(any_, any_),
            scratch_shapes=[V((wl, N), f32), DMA((N // pick(N, (256, 128)) + 1,))],
            compiler_params=pltpu.CompilerParams(vmem_limit_bytes=8 * 1024 * 1024),
        )(*[pltpu.with_memory_space_constraint(o, V) for o in outs])

    return jax.shard_map(
        per_device,
        mesh=mesh,
        in_specs=(
            P("section", None, "fsdp", None),
            P("section", "fsdp", None),
            P(None, "fsdp", None),
            P("section", None),
            P("section", None),
            P("section", "fsdp", "tp"),
        ),
        out_specs=(P("section", "fsdp", None), P("section", "fsdp", "tp")),
        check_vma=False,
    )
```

```python
import functools
import math

import jax
import jax.numpy as jnp
from jax import lax
from jax.experimental import pallas as pl
from jax.experimental.pallas import tpu as pltpu
from jax.sharding import PartitionSpec as P

norm_eps = 1e-06
MESH = pl.DeviceIdType.MESH
f32 = jnp.float32
bf16 = jnp.bfloat16
LAG = 3


def gelu_parts(u):
    k = 0.7978845608028654
    c = 0.044715
    u2 = u * u
    t = jnp.tanh(k * u * (1.0 + c * u2))
    half = 0.5 * (1.0 + t)
    act = u * half
    slope = half + 0.5 * u * (1.0 - t * t) * (k * (1.0 + 3.0 * c * u2))
    return act, slope


def pick(extent, options):
    for o in options:
        if extent % o == 0:
            return o
    return extent


def w_cuts(wl):
    if wl % 64 or wl <= 128:
        return (0, wl)
    deep = wl // 128 * 128
    cuts = list(range(0, deep, 256)) + [deep]
    return tuple(cuts) if deep == wl else tuple(cuts) + (wl,)


def row_step(wl):
    return math.gcd(wl, 64)


def kernel(
    S, FS, TP, T, order_in, gain_in, stash_ref, gnow_ref, gtop_ref, w_ref,
    held_ref, acc, lta, rhs,
    order_ref, gain_ref, wfull, stash, act, xt, inv, dyn, lt, prod, slope, own_e, peer_e, dxs, zin,
    lsem, topsem, w_s, w_r, l_s, l_r, r_s, r_r, e_s, e_r, z_r, x_s, x_r,
):
    s = lax.axis_index("section")
    f = lax.axis_index("fsdp")
    p = lax.axis_index("tp")
    NC = FS // 2
    SPLIT = (0, 1, 2)
    yc = f // 2
    core = f % 2
    sib = 2 * yc + (1 - core)
    n, D = act.shape[0] // (T + 1), act.shape[1]
    wl, N = w_ref.shape[1], w_ref.shape[2]
    cuts = w_cuts(wl)
    WCH = len(cuts) - 1
    wq = wl // TP
    CW = D // e_s.shape[-1]
    CH = D // CW
    nw = pick(N, (256, 128))
    tiles = N // nw
    here = CH * s // S
    there = CH * (s + 1) // S
    free = jnp.maximum(here, CH - there)

    loads = [
        pltpu.make_async_copy(w_ref.at[0], wfull.at[pl.ds(f * wl, wl), :], lsem.at[0]),
        pltpu.make_async_copy(stash_ref.at[0], stash, lsem.at[1]),
        pltpu.make_async_copy(gnow_ref.at[0], act.at[pl.ds(T * n, n), :], lsem.at[2]),
        pltpu.make_async_copy(order_in, order_ref, lsem.at[3]),
        pltpu.make_async_copy(gain_in, gain_ref, lsem.at[4]),
    ]
    for c in loads:
        c.start()

    bar = pltpu.get_barrier_semaphore()
    for r in range(1, FS):
        pl.semaphore_signal(bar, inc=1, device_id={"fsdp": (f + r) % FS}, device_id_type=MESH)
    for r in range(1, TP):
        pl.semaphore_signal(bar, inc=1, device_id={"tp": (p + r) % TP}, device_id_type=MESH)

    @pl.when(s > 0)
    def _():
        pl.semaphore_signal(bar, inc=1, device_id={"section": s - 1}, device_id_type=MESH)

    @pl.when(s < S - 1)
    def _():
        pl.semaphore_signal(bar, inc=1, device_id={"section": s + 1}, device_id_type=MESH)

    pl.semaphore_wait(bar, FS - 1 + TP - 1 + jnp.minimum(s, 1) + jnp.minimum(S - 1 - s, 1))

    def rcopy(src, dst, ss, rs, dev):
        return pltpu.make_async_remote_copy(
            src_ref=src, dst_ref=dst, send_sem=ss, recv_sem=rs, device_id=dev, device_id_type=MESH
        )

    def w_copy(k, j):
        lo, hi = cuts[j], cuts[j + 1]
        at = pl.multiple_of(lo + core * (wl - hi - lo), row_step(wl))
        if k < NC:
            rows = pl.ds(pl.multiple_of(f * wl + at, row_step(wl)), hi - lo)
            to = 2 * ((yc + k) % NC) + core
        else:
            o = k - NC + 1
            rows = pl.ds(pl.multiple_of((2 * ((yc - o + NC) % NC) + core) * wl + at, row_step(wl)), hi - lo)
            to = sib
        blk = wfull.at[rows, :]
        return rcopy(blk, blk, w_s.at[0], w_r.at[1 + (k - 1) * WCH + j], {"fsdp": to})

    def w_sib():
        blk = wfull.at[pl.ds(pl.multiple_of(f * wl, row_step(wl)), wl), :]
        return rcopy(blk, blk, w_s.at[0], w_r.at[0], {"fsdp": sib})

    loads[0].wait()
    for k in range(1, NC):
        for j in range(WCH):
            w_copy(k, j).start()
    w_sib().start()

    def is_split(part):
        return part in SPLIT and TP > 1

    def l_copy(part, k):
        cols = pl.ds(pl.multiple_of(f * n, n), n)
        if k == 0:
            to = sib
        else:
            o, cc = (k + 1) // 2, (k - 1) % 2
            to = 2 * ((yc + o) % NC) + (core + cc) % 2
        if k > 0 and is_split(part):
            src = lt.at[part, pl.ds(to * wl + p * wq, wq), :]
            dst = lta.at[part, pl.ds(p * wq, wq), cols]
        else:
            src = lt.at[part, pl.ds(to * wl, wl), :]
            dst = lta.at[part, :, cols]
        return rcopy(src, dst, l_s.at[part], l_r.at[part, min(k, 1)], {"fsdp": to})

    def x_copy(part, k, q):
        o, cc = (k + 1) // 2, (k - 1) % 2
        src_f = 2 * ((yc - o + NC) % NC) + (core + cc) % 2
        blk = lta.at[part, pl.ds(p * wq, wq), pl.ds(pl.multiple_of(src_f * n, n), n)]
        return rcopy(blk, blk, x_s.at[part], x_r.at[part], {"tp": (p + q) % TP})

    passed = set()

    def l_pass(part):
        if part in passed or not is_split(part):
            return
        passed.add(part)
        l_forward(part)

    def l_forward(part):
        l_far(part).wait_recv()
        for k in range(1, FS - 1):
            for q in range(1, TP):
                x_copy(part, k, q).start()

    def rows_of(part, rows, ss, rs):
        blk = lt.at[part, pl.ds(0, rows), :]
        return rcopy(blk, blk, ss, rs, {"fsdp": sib})

    def l_far(part):
        return rows_of(part, (FS - 2) * (wq if is_split(part) else wl), l_s.at[part], l_r.at[part, 1])

    def l_sent(part):
        return rows_of(part, wl + (FS - 2) * (wq if is_split(part) else wl), l_s.at[part], l_r.at[part, 1])

    def x_all(part):
        return rows_of(part, (FS - 2) * (TP - 1) * wq, x_s.at[part], x_r.at[part])

    def r_rows(part, count, which):
        blk = rhs.at[part, pl.ds(0, count * n), :]
        return rcopy(blk, blk, r_s.at[part], r_r.at[part, which], {"fsdp": sib})

    def l_send(part):
        for k in list(range(1, FS - 1)) + [0]:
            l_copy(part, k).start()
        lta[part, :, pl.ds(pl.multiple_of(f * n, n), n)] = lt[part, pl.ds(pl.multiple_of(f * wl, row_step(wl)), wl), :]

    def r_copy(part, k):
        if k < NC:
            at = f
            to = sib if k == 0 else 2 * ((yc + k) % NC) + core
        else:
            o = k - NC + 1
            at = 2 * ((yc - o + NC) % NC) + core
            to = sib
        blk = rhs.at[part, pl.ds(pl.multiple_of(at * n, n), n), :]
        return rcopy(blk, blk, r_s.at[part], r_r.at[part, k if 0 < k < NC else 0], {"fsdp": to})

    def r_send(part):
        for k in list(range(1, NC)) + [0]:
            r_copy(part, k).start()

    tw = pick(D, (256, 128))

    def transpose_rows(part, ref, first):
        @pl.loop(0, D // tw)
        def _(i):
            cols = pl.ds(pl.multiple_of(i * tw, tw), tw)
            lt[part, cols, :] = ref[pl.ds(first, n), cols].astype(f32).T.astype(bf16)

    loads[3].wait()
    loads[4].wait()
    loads[1].wait()
    rb = pick(n, (32, 16))
    for t in range(T):
        slot = order_ref[0, t]

        @pl.loop(0, n // rb)
        def _(i):
            rows = pl.ds(pl.multiple_of(i * rb, rb), rb)
            raw = stash[slot, rows, :]
            v = raw.astype(f32)
            iv = lax.rsqrt(jnp.mean(v * v, axis=-1, keepdims=True) + norm_eps)
            xt[t, rows, :] = raw
            inv[t, rows, :] = jnp.broadcast_to(iv, (rb, 128))
            act[pl.ds(pl.multiple_of(t * n + i * rb, rb), rb), :] = ((v * iv) * gain_ref[0:1, :]).astype(bf16)

        transpose_rows(2 * t, act, t * n)
        if t == 0:
            l_send(0)
            loads[2].wait()
            transpose_rows(1, act, T * n)
            l_send(1)
        else:
            l_send(2 * t)

    @pl.when(s == S - 1)
    def _():
        for t in range(T):
            pltpu.make_async_copy(gtop_ref.at[t], zin.at[t], topsem.at[t]).start()

    half = 2 * wl

    def part_product(chip, spans, first):
        @pl.loop(0, tiles)
        def _(i):
            cols = pl.ds(pl.multiple_of(i * nw, nw), nw)
            d = None
            for lo, hi in spans:
                ks = pl.ds(pl.multiple_of(chip * half + lo, math.gcd(half, lo)), hi - lo)
                one = jnp.dot(act[:, ks], wfull[ks, cols], preferred_element_type=f32)
                d = one if d is None else d + one
            if first:
                prod[:, cols] = d
            else:
                prod[:, cols] += d

    w_sib().wait_recv()
    part_product(yc, [(0, half)], True)
    for o in range(1, NC):
        for j in range(WCH):
            w_copy(o, j).wait_recv()
            w_copy(NC - 1 + o, j).start()
            w_copy(NC - 1 + o, j).wait_recv()
            lo, hi = cuts[j], cuts[j + 1]
            spans = [(lo, half - lo)] if hi == wl else [(lo, hi), (half - hi, half - lo)]
            part_product((yc - o + NC) % NC, spans, False)

    mine = pl.multiple_of(f * n, n)

    def gelu_rows(t, with_grad):
        @pl.loop(0, n // rb)
        def _(i):
            rows = pl.ds(pl.multiple_of(t * n + i * rb, rb), rb)
            home = pl.ds(pl.multiple_of(mine + i * rb, rb), rb)
            a, sl = gelu_parts(prod[rows, :])
            rhs[2 * t + 1, home, :] = a.astype(bf16)
            if with_grad:
                g = prod[pl.ds(pl.multiple_of(T * n + i * rb, rb), rb), :]
                rhs[2 * t, home, :] = (sl * g).astype(bf16)
            else:
                slope[t, pl.ds(pl.multiple_of(i * rb, rb), rb), :] = sl

    def e_copy(t, r, c):
        cols = pl.ds(pl.multiple_of(c * CW, CW), CW)
        return rcopy(
            own_e.at[t, :, cols], peer_e.at[t, r - 1, :, cols],
            e_s.at[t, c], e_r.at[t, r - 1, c], {"tp": (p + r) % TP},
        )

    def f_copy(t, r, c):
        cols = pl.ds(pl.multiple_of(c * CW, CW), CW)
        return rcopy(
            zin.at[t, :, cols], peer_e.at[t, r - 1, :, cols],
            e_s.at[t, c], e_r.at[t, r - 1, c], {"tp": (p + r) % TP},
        )

    def z_copy(t, c, src):
        cols = pl.ds(pl.multiple_of(c * CW, CW), CW)
        to = jnp.maximum(s - 1, 0)
        return rcopy(
            src.at[t, :, cols], zin.at[t, :, cols], e_s.at[t, c], z_r.at[t, c], {"section": to}
        )

    def held_dy(t, cols):
        return (act[pl.ds(T * n, n), cols] if t == 0 else dyn[t - 1, :, cols]).astype(f32)

    def spread(t):
        du = rhs[2 * t, pl.ds(mine, n), :]
        u = prod[pl.ds(t * n, n), :]
        m = jnp.sum(du.astype(f32) * u, axis=-1, keepdims=True) / D
        iv = inv[t, :, 0:1]
        q_scale = iv * iv * m

        @pl.loop(0, CH)
        def _(i):
            both = jnp.minimum(here, CH - here)
            far_turn = jnp.where(i < 2 * both, i % 2 == 0, CH - here > here)
            turn = jnp.where(i < 2 * both, i // 2, i - both)
            c = jnp.where(far_turn, CH - 1 - turn, here - 1 - turn)
            cols = pl.ds(pl.multiple_of(c * CW, CW), CW)
            dh = lax.dot_general(
                rhs[2 * t, pl.ds(mine, n), :], wfull[cols, :], (((1,), (1,)), ((), ())),
                preferred_element_type=f32,
            )
            e = iv * (gain_ref[0:1, cols] * dh) - xt[t, :, cols].astype(f32) * q_scale
            own_e[t, :, cols] = jnp.where((c >= here) & (p == 0), e + held_dy(t, cols), e).astype(bf16)

            @pl.when(c >= here)
            def _():
                z_copy(t, c, own_e).start()

            @pl.when(c < here)
            def _():
                for r in range(1, TP):
                    e_copy(t, r, c).start()

    def combine(t, c):
        cols = pl.ds(pl.multiple_of(c * CW, CW), CW)
        for r in range(1, TP):
            e_copy(t, r, c).wait_recv()
        total = own_e[t, :, cols].astype(f32)
        for r in range(1, TP):
            total = total + peer_e[t, r - 1, :, cols].astype(f32)
        dxs[t, :, cols] = (held_dy(t, cols) + total).astype(bf16)
        z_copy(t, c, dxs).start()

    def forward(t, c):
        z_copy(t, c, dxs).wait_recv()
        for r in range(1, TP):
            f_copy(t, r, c).start()

    def put(t, cols, value):
        if t == T - 1:
            held_ref[0, :, cols] = value
        else:
            dyn[t, :, cols] = value

    def arrive(t, c):
        cols = pl.ds(pl.multiple_of(c * CW, CW), CW)

        @pl.when((c < there) & (s < S - 1))
        def _():
            z_copy(t, c, dxs).wait_recv()

        @pl.when(c < there)
        def _():
            put(t, cols, zin[t, :, cols])

        @pl.when(c >= there)
        def _():
            total = zin[t, :, cols].astype(f32)
            for r in range(1, TP):
                f_copy(t, r, c).wait_recv()
                total = total + peer_e[t, r - 1, :, cols].astype(f32)
            put(t, cols, total.astype(bf16))

        return cols

    def relay_loop(t, consume, service):
        @pl.loop(0, CH + LAG)
        def _(i):
            @pl.when(i < CH - there)
            def _():
                forward(t, CH - 1 - i)

            @pl.when(i < here)
            def _():
                combine(t, here - 1 - i)

            service(i)

            @pl.when(i >= LAG)
            def _():
                j = i - LAG
                consume(j, CH - 1 - j)

    def at_step(i, step, fn):
        @pl.when(i == step)
        def _():
            fn()

    relayed = set()

    def r_relay(part):
        if part in relayed:
            return
        relayed.add(part)
        for o in range(1, NC):
            r_copy(part, o).wait_recv()
            r_copy(part, NC - 1 + o).start()

    parts = []
    for t in range(T):
        parts += [2 * t, 2 * t + 1]

    def own_wait(part):
        l_copy(part, 0).wait_recv()
        if is_split(part):
            x_all(part).wait_recv()
        elif FS > 2:
            l_far(part).wait_recv()
        r_rows(part, NC, 0).wait_recv()

    def own_tile(at, i):
        part = parts[at]
        cols = pl.ds(pl.multiple_of(i * nw, nw), nw)
        d = jnp.dot(lta[part], rhs[part, :, cols], preferred_element_type=f32)
        if at > 0:
            d = acc[:, cols] + d
        acc[:, cols] = d

    def sent():
        w_rows = wfull.at[pl.ds(0, (2 * NC - 1) * wl), :]
        rcopy(w_rows, w_rows, w_s.at[0], w_r.at[0], {"fsdp": sib}).wait_send()
        for part in range(2 * T):
            l_sent(part).wait_send()
            if is_split(part) and FS > 2:
                x_all(part).wait_send()
        for t in range(T):
            @pl.loop(0, CH)
            def _(c):
                crossed = (c < here) | (c >= there)

                @pl.when(crossed & (s > 0))
                def _():
                    chunk_sent(t, c, TP)

                @pl.when(crossed & (s == 0))
                def _():
                    chunk_sent(t, c, TP - 1)

                @pl.when(jnp.logical_not(crossed) & (s > 0))
                def _():
                    chunk_sent(t, c, 1)

    def chunk_sent(t, c, count):
        blk = own_e.at[t, :, pl.ds(0, count * CW)]
        if count > 0:
            rcopy(blk, blk, e_s.at[t, c], z_r.at[t, c], {"fsdp": sib}).wait_send()

    for t in range(T):
        last = t == T - 1
        if t == 0:
            gelu_rows(0, True)
            r_send(0)
            r_send(1)
        else:
            r_send(2 * t)
            l_send(2 * t + 1)

        @pl.when(s > 0)
        def _():
            spread(t)

        if t == 0:
            for later in range(1, T):
                gelu_rows(later, False)
                r_send(2 * later + 1)

        @pl.when(s == S - 1)
        def _():
            pltpu.make_async_copy(gtop_ref.at[t], zin.at[t], topsem.at[t]).wait()

        if not last:
            gr = pl.ds(T * n, n)

            def consume(j, c):
                cols = arrive(t, c)
                d = dyn[t, :, cols]
                lt[2 * t + 3, cols, :] = d.astype(f32).T.astype(bf16)
                g = jnp.dot(d, wfull[cols, :], preferred_element_type=f32)

                @pl.when(j == 0)
                def _():
                    prod[gr, :] = g

                @pl.when(j > 0)
                def _():
                    prod[gr, :] += g

            def service(i):
                if t == 0:
                    if is_split(0):
                        passed.add(0)
                        at_step(i, jnp.where(s == 0, -1, free), lambda: l_forward(0))
                    at_step(i, free, lambda: l_pass(1))
                    at_step(i, CH + LAG - 1, lambda: r_relay(0))
                    if is_split(2):
                        at_step(i, jnp.where(s == 0, CH + LAG - 1, -1), lambda: l_forward(2))

            if t == 0 and is_split(0):
                @pl.when(s == 0)
                def _():
                    l_forward(0)

            relay_loop(t, consume, service)

            @pl.loop(0, n // rb)
            def _(i):
                rows = pl.ds(pl.multiple_of(i * rb, rb), rb)
                g = prod[pl.ds(pl.multiple_of(T * n + i * rb, rb), rb), :]
                here_rows = pl.ds(pl.multiple_of(mine + i * rb, rb), rb)
                rhs[2 * t + 2, here_rows, :] = (slope[t + 1, rows, :] * g).astype(bf16)
        else:
            late = len(parts) - 1
            steps = CH + LAG

            def consume(j, c):
                arrive(t, c)

            def begin(at):
                part = parts[at]
                l_pass(part)
                r_relay(part)
                own_wait(part)

            def service(i):
                if late > 2:
                    at_step(i, 0, lambda: r_relay(parts[1]))
                    if is_split(2):
                        passed.add(2)
                        at_step(i, jnp.where(s == 0, -1, free), lambda: l_forward(2))
                    at_step(i, CH - 1, lambda: (r_relay(parts[late]), r_relay(parts[2])))
                for k in range(late):
                    first = k * tiles + (k > 1)

                    @pl.when((i >= first) & (i < first + tiles))
                    def _():
                        @pl.when(i == first)
                        def _():
                            begin(k)

                        own_tile(k, i - first)

            relay_loop(t, consume, service)
            for k in range(late):
                first = k * tiles + (k > 1)
                if first >= steps:
                    begin(k)
                for i in range(max(steps - first, 0), tiles):
                    own_tile(k, i)
            sent()
            begin(late)

    for part in range(2 * T):
        r_rows(part, 2 * NC - 1, 0).wait_send()


def finish(part, held_in, acc, lta, rhs, held_ref, wg_ref, grad, sem):
    N = acc.shape[1]
    nw = pick(N, (256, 128))
    tiles = N // nw
    held = pltpu.make_async_copy(held_in, held_ref, sem.at[tiles])
    held.start()

    def tile_copy(i):
        cols = pl.ds(i * nw, nw)
        return pltpu.make_async_copy(grad.at[:, cols], wg_ref.at[0, :, cols], sem.at[i])

    for i in range(tiles):
        cols = pl.ds(i * nw, nw)
        grad[:, cols] = acc[:, cols] + jnp.dot(lta[part], rhs[part, :, cols], preferred_element_type=f32)
        tile_copy(i).start()
    for i in range(tiles):
        tile_copy(i).wait()
    held.wait()


def solution(mesh):
    S, FS, TP = mesh.shape["section"], mesh.shape["fsdp"], mesh.shape["tp"]

    def per_device(stash, grad_now, grad_top, order, gain, weight):
        MB, n, D = stash.shape[1:]
        T = grad_top.shape[0]
        wl, N = weight.shape[1:]
        NC = FS // 2
        CH = D // pick(D, (256, 128))
        WCH = len(w_cuts(wl)) - 1
        K = 2 * NC - 1
        DMA = pltpu.SemaphoreType.DMA
        V = pltpu.VMEM
        any_ = pl.BlockSpec(memory_space=pl.ANY)
        vmem = pl.BlockSpec(memory_space=V)
        peers = max(TP - 1, 1)
        outs = pl.pallas_call(
            functools.partial(kernel, S, FS, TP, T),
            out_shape=(
                V((1, n, D), bf16),
                V((wl, N), f32),
                V((2 * T, wl, FS * n), bf16),
                V((2 * T, FS * n, N), bf16),
            ),
            in_specs=[
                any_, any_, any_, any_, any_, any_,
            ],
            out_specs=(vmem,) * 4,
            scratch_shapes=[
                pltpu.SMEM((1, MB), jnp.int32),
                V((1, D), f32),
                V((FS * wl, N), bf16),
                V((MB, n, D), bf16),
                V(((T + 1) * n, D), bf16),
                V((T, n, D), bf16),
                V((T, n, 128), f32),
                V((T, n, D), bf16),
                V((2 * T, D, n), bf16),
                V(((T + 1) * n, N), f32),
                V((T, n, N), f32),
                V((T, n, D), bf16),
                V((T, peers, n, D), bf16),
                V((T, n, D), bf16),
                V((T, n, D), bf16),
                DMA((5,)), DMA((T,)),
                DMA((1,)), DMA((1 + (K - 1) * WCH,)),
                DMA((2 * T,)), DMA((2 * T, 2)),
                DMA((2 * T,)), DMA((2 * T, NC)),
                DMA((T, CH)), DMA((T, peers, CH)), DMA((T, CH)),
                DMA((2 * T,)), DMA((2 * T,)),
            ],
            compiler_params=pltpu.CompilerParams(
                collective_id=0, has_side_effects=True, vmem_limit_bytes=44 * 1024 * 1024
            ),
        )(*[pltpu.with_memory_space_constraint(o, pltpu.HBM) for o in (order, gain, stash, grad_now, grad_top, weight)])
        return pl.pallas_call(
            functools.partial(finish, 2 * T - 1),
            out_shape=(
                jax.ShapeDtypeStruct((1, n, D), bf16),
                jax.ShapeDtypeStruct((1, wl, N), f32),
            ),
            in_specs=[vmem] * 4,
            out_specs=(any_, any_),
            scratch_shapes=[V((wl, N), f32), DMA((N // pick(N, (256, 128)) + 1,))],
            compiler_params=pltpu.CompilerParams(vmem_limit_bytes=8 * 1024 * 1024),
        )(*[pltpu.with_memory_space_constraint(o, V) for o in outs])

    return jax.shard_map(
        per_device,
        mesh=mesh,
        in_specs=(
            P("section", None, "fsdp", None),
            P("section", "fsdp", None),
            P(None, "fsdp", None),
            P("section", None),
            P("section", None),
            P("section", "fsdp", "tp"),
        ),
        out_specs=(P("section", "fsdp", None), P("section", "fsdp", "tp")),
        check_vma=False,
    )
```

```python
import functools
import math

import jax
import jax.numpy as jnp
from jax import lax
from jax.experimental import pallas as pl
from jax.experimental.pallas import tpu as pltpu
from jax.sharding import PartitionSpec as P

norm_eps = 1e-06
MESH = pl.DeviceIdType.MESH
f32 = jnp.float32
bf16 = jnp.bfloat16
LAG = 3


def gelu_parts(u):
    k = 0.7978845608028654
    c = 0.044715
    u2 = u * u
    t = jnp.tanh(k * u * (1.0 + c * u2))
    half = 0.5 * (1.0 + t)
    act = u * half
    slope = half + 0.5 * u * (1.0 - t * t) * (k * (1.0 + 3.0 * c * u2))
    return act, slope


def pick(extent, options):
    for o in options:
        if extent % o == 0:
            return o
    return extent


def w_cuts(wl):
    if wl % 64 or wl <= 128:
        return (0, wl)
    deep = wl // 128 * 128
    cuts = list(range(0, deep, 256)) + [deep]
    return tuple(cuts) if deep == wl else tuple(cuts) + (wl,)


def row_step(wl):
    return math.gcd(wl, 64)


def kernel(
    S, FS, TP, T, order_in, gain_in, stash_ref, gnow_ref, gtop_ref, w_ref,
    held_ref, acc, lta, rhs,
    order_ref, gain_ref, wfull, stash, act, xt, inv, dyn, lt, prod, slope, own_e, peer_e, dxs, zin,
    lsem, topsem, w_s, w_r, l_s, l_r, r_s, r_r, e_s, e_r, z_r, x_s, x_r,
):
    s = lax.axis_index("section")
    f = lax.axis_index("fsdp")
    p = lax.axis_index("tp")
    NC = FS // 2
    SPLIT = (0, 1, 2)
    yc = f // 2
    core = f % 2
    sib = 2 * yc + (1 - core)
    n, D = act.shape[0] // (T + 1), act.shape[1]
    wl, N = w_ref.shape[1], w_ref.shape[2]
    cuts = w_cuts(wl)
    WCH = len(cuts) - 1
    wq = wl // TP
    CW = D // e_s.shape[-1]
    CH = D // CW
    nw = pick(N, (256, 128))
    tiles = N // nw
    here = CH * s // S
    there = CH * (s + 1) // S
    free = jnp.maximum(here, CH - there)

    loads = [
        pltpu.make_async_copy(w_ref.at[0], wfull.at[pl.ds(f * wl, wl), :], lsem.at[0]),
        pltpu.make_async_copy(stash_ref.at[0], stash, lsem.at[1]),
        pltpu.make_async_copy(gnow_ref.at[0], act.at[pl.ds(T * n, n), :], lsem.at[2]),
        pltpu.make_async_copy(order_in, order_ref, lsem.at[3]),
        pltpu.make_async_copy(gain_in, gain_ref, lsem.at[4]),
    ]
    for c in loads:
        c.start()

    bar = pltpu.get_barrier_semaphore()
    for r in range(1, FS):
        pl.semaphore_signal(bar, inc=1, device_id={"fsdp": (f + r) % FS}, device_id_type=MESH)
    for r in range(1, TP):
        pl.semaphore_signal(bar, inc=1, device_id={"tp": (p + r) % TP}, device_id_type=MESH)

    @pl.when(s > 0)
    def _():
        pl.semaphore_signal(bar, inc=1, device_id={"section": s - 1}, device_id_type=MESH)

    @pl.when(s < S - 1)
    def _():
        pl.semaphore_signal(bar, inc=1, device_id={"section": s + 1}, device_id_type=MESH)

    pl.semaphore_wait(bar, FS - 1 + TP - 1 + jnp.minimum(s, 1) + jnp.minimum(S - 1 - s, 1))

    def rcopy(src, dst, ss, rs, dev):
        return pltpu.make_async_remote_copy(
            src_ref=src, dst_ref=dst, send_sem=ss, recv_sem=rs, device_id=dev, device_id_type=MESH
        )

    def w_copy(k, j):
        lo, hi = cuts[j], cuts[j + 1]
        at = pl.multiple_of(lo + core * (wl - hi - lo), row_step(wl))
        if k < NC:
            rows = pl.ds(pl.multiple_of(f * wl + at, row_step(wl)), hi - lo)
            to = 2 * ((yc + k) % NC) + core
        else:
            o = k - NC + 1
            rows = pl.ds(pl.multiple_of((2 * ((yc - o + NC) % NC) + core) * wl + at, row_step(wl)), hi - lo)
            to = sib
        blk = wfull.at[rows, :]
        return rcopy(blk, blk, w_s.at[0], w_r.at[1 + (k - 1) * WCH + j], {"fsdp": to})

    def w_sib():
        blk = wfull.at[pl.ds(pl.multiple_of(f * wl, row_step(wl)), wl), :]
        return rcopy(blk, blk, w_s.at[0], w_r.at[0], {"fsdp": sib})

    loads[0].wait()
    for k in range(1, NC):
        for j in range(WCH):
            w_copy(k, j).start()
    w_sib().start()

    def is_split(part):
        return part in SPLIT and TP > 1

    def l_copy(part, k):
        cols = pl.ds(pl.multiple_of(f * n, n), n)
        if k == 0:
            to = sib
        else:
            o, cc = (k + 1) // 2, (k - 1) % 2
            to = 2 * ((yc + o) % NC) + (core + cc) % 2
        if k > 0 and is_split(part):
            src = lt.at[part, pl.ds(to * wl + p * wq, wq), :]
            dst = lta.at[part, pl.ds(p * wq, wq), cols]
        else:
            src = lt.at[part, pl.ds(to * wl, wl), :]
            dst = lta.at[part, :, cols]
        return rcopy(src, dst, l_s.at[part], l_r.at[part, min(k, 1)], {"fsdp": to})

    def x_copy(part, k, q):
        o, cc = (k + 1) // 2, (k - 1) % 2
        src_f = 2 * ((yc - o + NC) % NC) + (core + cc) % 2
        blk = lta.at[part, pl.ds(p * wq, wq), pl.ds(pl.multiple_of(src_f * n, n), n)]
        return rcopy(blk, blk, x_s.at[part], x_r.at[part], {"tp": (p + q) % TP})

    passed = set()

    def l_pass(part):
        if part in passed or not is_split(part):
            return
        passed.add(part)
        l_forward(part)

    def l_forward(part):
        l_far(part).wait_recv()
        for k in range(1, FS - 1):
            for q in range(1, TP):
                x_copy(part, k, q).start()

    def rows_of(part, rows, ss, rs):
        blk = lt.at[part, pl.ds(0, rows), :]
        return rcopy(blk, blk, ss, rs, {"fsdp": sib})

    def l_far(part):
        return rows_of(part, (FS - 2) * (wq if is_split(part) else wl), l_s.at[part], l_r.at[part, 1])

    def l_sent(part):
        return rows_of(part, wl + (FS - 2) * (wq if is_split(part) else wl), l_s.at[part], l_r.at[part, 1])

    def x_all(part):
        return rows_of(part, (FS - 2) * (TP - 1) * wq, x_s.at[part], x_r.at[part])

    def r_rows(part, count, which):
        blk = rhs.at[part, pl.ds(0, count * n), :]
        return rcopy(blk, blk, r_s.at[part], r_r.at[part, which], {"fsdp": sib})

    def l_send(part):
        for k in list(range(1, FS - 1)) + [0]:
            l_copy(part, k).start()
        lta[part, :, pl.ds(pl.multiple_of(f * n, n), n)] = lt[part, pl.ds(pl.multiple_of(f * wl, row_step(wl)), wl), :]

    def r_copy(part, k):
        if k < NC:
            at = f
            to = sib if k == 0 else 2 * ((yc + k) % NC) + core
        else:
            o = k - NC + 1
            at = 2 * ((yc - o + NC) % NC) + core
            to = sib
        blk = rhs.at[part, pl.ds(pl.multiple_of(at * n, n), n), :]
        return rcopy(blk, blk, r_s.at[part], r_r.at[part, k if 0 < k < NC else 0], {"fsdp": to})

    def r_send(part):
        for k in list(range(1, NC)) + [0]:
            r_copy(part, k).start()

    tw = pick(D, (256, 128))

    def transpose_rows(part, ref, first):
        @pl.loop(0, D // tw)
        def _(i):
            cols = pl.ds(pl.multiple_of(i * tw, tw), tw)
            lt[part, cols, :] = ref[pl.ds(first, n), cols].astype(f32).T.astype(bf16)

    loads[3].wait()
    loads[4].wait()
    loads[1].wait()
    rb = pick(n, (32, 16))
    for t in range(T):
        slot = order_ref[0, t]

        @pl.loop(0, n // rb)
        def _(i):
            rows = pl.ds(pl.multiple_of(i * rb, rb), rb)
            raw = stash[slot, rows, :]
            v = raw.astype(f32)
            iv = lax.rsqrt(jnp.mean(v * v, axis=-1, keepdims=True) + norm_eps)
            xt[t, rows, :] = raw
            inv[t, rows, :] = jnp.broadcast_to(iv, (rb, 128))
            act[pl.ds(pl.multiple_of(t * n + i * rb, rb), rb), :] = ((v * iv) * gain_ref[0:1, :]).astype(bf16)

        transpose_rows(2 * t, act, t * n)
        if t == 0:
            l_send(0)
            loads[2].wait()
            transpose_rows(1, act, T * n)
            l_send(1)
        else:
            l_send(2 * t)

    @pl.when(s == S - 1)
    def _():
        for t in range(T):
            pltpu.make_async_copy(gtop_ref.at[t], zin.at[t], topsem.at[t]).start()

    half = 2 * wl

    def part_product(chip, spans, first, width):
        @pl.loop(0, N // width)
        def _(i):
            cols = pl.ds(pl.multiple_of(i * width, width), width)
            d = None
            for lo, hi in spans:
                ks = pl.ds(pl.multiple_of(chip * half + lo, math.gcd(half, lo)), hi - lo)
                one = jnp.dot(act[:, ks], wfull[ks, cols], preferred_element_type=f32)
                d = one if d is None else d + one
            if first:
                prod[:, cols] = d
            else:
                prod[:, cols] += d

    w_sib().wait_recv()
    part_product(yc, [(0, half)], True, nw)
    for o in range(1, NC):
        for j in range(WCH):
            w_copy(o, j).wait_recv()
            w_copy(NC - 1 + o, j).start()
            w_copy(NC - 1 + o, j).wait_recv()
            lo, hi = cuts[j], cuts[j + 1]
            spans = [(lo, half - lo)] if hi == wl else [(lo, hi), (half - hi, half - lo)]
            part_product((yc - o + NC) % NC, spans, False, N if hi == wl and 0 < lo else nw)

    mine = pl.multiple_of(f * n, n)

    def gelu_rows(t, with_grad):
        @pl.loop(0, n // rb)
        def _(i):
            rows = pl.ds(pl.multiple_of(t * n + i * rb, rb), rb)
            home = pl.ds(pl.multiple_of(mine + i * rb, rb), rb)
            a, sl = gelu_parts(prod[rows, :])
            rhs[2 * t + 1, home, :] = a.astype(bf16)
            if with_grad:
                g = prod[pl.ds(pl.multiple_of(T * n + i * rb, rb), rb), :]
                rhs[2 * t, home, :] = (sl * g).astype(bf16)
            else:
                slope[t, pl.ds(pl.multiple_of(i * rb, rb), rb), :] = sl

    def e_copy(t, r, c):
        cols = pl.ds(pl.multiple_of(c * CW, CW), CW)
        return rcopy(
            own_e.at[t, :, cols], peer_e.at[t, r - 1, :, cols],
            e_s.at[t, c], e_r.at[t, r - 1, c], {"tp": (p + r) % TP},
        )

    def f_copy(t, r, c):
        cols = pl.ds(pl.multiple_of(c * CW, CW), CW)
        return rcopy(
            zin.at[t, :, cols], peer_e.at[t, r - 1, :, cols],
            e_s.at[t, c], e_r.at[t, r - 1, c], {"tp": (p + r) % TP},
        )

    def z_copy(t, c, src):
        cols = pl.ds(pl.multiple_of(c * CW, CW), CW)
        to = jnp.maximum(s - 1, 0)
        return rcopy(
            src.at[t, :, cols], zin.at[t, :, cols], e_s.at[t, c], z_r.at[t, c], {"section": to}
        )

    def held_dy(t, cols):
        return (act[pl.ds(T * n, n), cols] if t == 0 else dyn[t - 1, :, cols]).astype(f32)

    def spread(t):
        du = rhs[2 * t, pl.ds(mine, n), :]
        u = prod[pl.ds(t * n, n), :]
        m = jnp.sum(du.astype(f32) * u, axis=-1, keepdims=True) / D
        iv = inv[t, :, 0:1]
        q_scale = iv * iv * m

        @pl.loop(0, CH)
        def _(i):
            both = jnp.minimum(here, CH - here)
            far_turn = jnp.where(i < 2 * both, i % 2 == 0, CH - here > here)
            turn = jnp.where(i < 2 * both, i // 2, i - both)
            c = jnp.where(far_turn, CH - 1 - turn, here - 1 - turn)
            cols = pl.ds(pl.multiple_of(c * CW, CW), CW)
            dh = lax.dot_general(
                rhs[2 * t, pl.ds(mine, n), :], wfull[cols, :], (((1,), (1,)), ((), ())),
                preferred_element_type=f32,
            )
            e = iv * (gain_ref[0:1, cols] * dh) - xt[t, :, cols].astype(f32) * q_scale
            own_e[t, :, cols] = jnp.where((c >= here) & (p == 0), e + held_dy(t, cols), e).astype(bf16)

            @pl.when(c >= here)
            def _():
                z_copy(t, c, own_e).start()

            @pl.when(c < here)
            def _():
                for r in range(1, TP):
                    e_copy(t, r, c).start()

    def combine(t, c):
        cols = pl.ds(pl.multiple_of(c * CW, CW), CW)
        for r in range(1, TP):
            e_copy(t, r, c).wait_recv()
        total = own_e[t, :, cols].astype(f32)
        for r in range(1, TP):
            total = total + peer_e[t, r - 1, :, cols].astype(f32)
        dxs[t, :, cols] = (held_dy(t, cols) + total).astype(bf16)
        z_copy(t, c, dxs).start()

    def forward(t, c):
        z_copy(t, c, dxs).wait_recv()
        for r in range(1, TP):
            f_copy(t, r, c).start()

    def put(t, cols, value):
        if t == T - 1:
            held_ref[0, :, cols] = value
        else:
            dyn[t, :, cols] = value

    def arrive(t, c):
        cols = pl.ds(pl.multiple_of(c * CW, CW), CW)

        @pl.when((c < there) & (s < S - 1))
        def _():
            z_copy(t, c, dxs).wait_recv()

        @pl.when(c < there)
        def _():
            put(t, cols, zin[t, :, cols])

        @pl.when(c >= there)
        def _():
            total = zin[t, :, cols].astype(f32)
            for r in range(1, TP):
                f_copy(t, r, c).wait_recv()
                total = total + peer_e[t, r - 1, :, cols].astype(f32)
            put(t, cols, total.astype(bf16))

        return cols

    def relay_loop(t, consume, service):
        @pl.loop(0, CH + LAG)
        def _(i):
            @pl.when(i < CH - there)
            def _():
                forward(t, CH - 1 - i)

            @pl.when(i < here)
            def _():
                combine(t, here - 1 - i)

            service(i)

            @pl.when(i >= LAG)
            def _():
                j = i - LAG
                consume(j, CH - 1 - j)

    def at_step(i, step, fn):
        @pl.when(i == step)
        def _():
            fn()

    relayed = set()

    def r_relay(part):
        if part in relayed:
            return
        relayed.add(part)
        for o in range(1, NC):
            r_copy(part, o).wait_recv()
            r_copy(part, NC - 1 + o).start()

    parts = []
    for t in range(T):
        parts += [2 * t, 2 * t + 1]

    def own_wait(part):
        l_copy(part, 0).wait_recv()
        if is_split(part):
            x_all(part).wait_recv()
        elif FS > 2:
            l_far(part).wait_recv()
        r_rows(part, NC, 0).wait_recv()

    def own_tile(at, i):
        part = parts[at]
        cols = pl.ds(pl.multiple_of(i * nw, nw), nw)
        d = jnp.dot(lta[part], rhs[part, :, cols], preferred_element_type=f32)
        if at > 0:
            d = acc[:, cols] + d
        acc[:, cols] = d

    def sent():
        w_rows = wfull.at[pl.ds(0, (2 * NC - 1) * wl), :]
        rcopy(w_rows, w_rows, w_s.at[0], w_r.at[0], {"fsdp": sib}).wait_send()
        for part in range(2 * T):
            l_sent(part).wait_send()
            if is_split(part) and FS > 2:
                x_all(part).wait_send()
        for t in range(T):
            @pl.loop(0, CH)
            def _(c):
                crossed = (c < here) | (c >= there)

                @pl.when(crossed & (s > 0))
                def _():
                    chunk_sent(t, c, TP)

                @pl.when(crossed & (s == 0))
                def _():
                    chunk_sent(t, c, TP - 1)

                @pl.when(jnp.logical_not(crossed) & (s > 0))
                def _():
                    chunk_sent(t, c, 1)

    def chunk_sent(t, c, count):
        blk = own_e.at[t, :, pl.ds(0, count * CW)]
        if count > 0:
            rcopy(blk, blk, e_s.at[t, c], z_r.at[t, c], {"fsdp": sib}).wait_send()

    for t in range(T):
        last = t == T - 1
        if t == 0:
            gelu_rows(0, True)
            r_send(0)
            r_send(1)
        else:
            r_send(2 * t)
            l_send(2 * t + 1)

        @pl.when(s > 0)
        def _():
            spread(t)

        if t == 0:
            for later in range(1, T):
                gelu_rows(later, False)
                r_send(2 * later + 1)

        @pl.when(s == S - 1)
        def _():
            pltpu.make_async_copy(gtop_ref.at[t], zin.at[t], topsem.at[t]).wait()

        if not last:
            gr = pl.ds(T * n, n)

            def consume(j, c):
                cols = arrive(t, c)
                d = dyn[t, :, cols]
                lt[2 * t + 3, cols, :] = d.astype(f32).T.astype(bf16)
                g = jnp.dot(d, wfull[cols, :], preferred_element_type=f32)

                @pl.when(j == 0)
                def _():
                    prod[gr, :] = g

                @pl.when(j > 0)
                def _():
                    prod[gr, :] += g

            def service(i):
                if t == 0:
                    if is_split(0):
                        passed.add(0)
                        at_step(i, jnp.where(s == 0, -1, free), lambda: l_forward(0))
                    at_step(i, free, lambda: l_pass(1))
                    at_step(i, CH + LAG - 1, lambda: r_relay(0))
                    if is_split(2):
                        at_step(i, jnp.where(s == 0, CH + LAG - 1, -1), lambda: l_forward(2))

            if t == 0 and is_split(0):
                @pl.when(s == 0)
                def _():
                    l_forward(0)

            relay_loop(t, consume, service)

            @pl.loop(0, n // rb)
            def _(i):
                rows = pl.ds(pl.multiple_of(i * rb, rb), rb)
                g = prod[pl.ds(pl.multiple_of(T * n + i * rb, rb), rb), :]
                here_rows = pl.ds(pl.multiple_of(mine + i * rb, rb), rb)
                rhs[2 * t + 2, here_rows, :] = (slope[t + 1, rows, :] * g).astype(bf16)
        else:
            late = len(parts) - 1
            steps = CH + LAG

            def consume(j, c):
                arrive(t, c)

            def begin(at):
                part = parts[at]
                l_pass(part)
                r_relay(part)
                own_wait(part)

            def service(i):
                if late > 2:
                    at_step(i, 0, lambda: r_relay(parts[1]))
                    if is_split(2):
                        passed.add(2)
                        at_step(i, jnp.where(s == 0, -1, free), lambda: l_forward(2))
                    at_step(i, CH - 1, lambda: (r_relay(parts[late]), r_relay(parts[2])))
                for k in range(late):
                    first = k * tiles + (k > 1)

                    @pl.when((i >= first) & (i < first + tiles))
                    def _():
                        @pl.when(i == first)
                        def _():
                            begin(k)

                        own_tile(k, i - first)

            relay_loop(t, consume, service)
            for k in range(late):
                first = k * tiles + (k > 1)
                if first >= steps:
                    begin(k)
                for i in range(max(steps - first, 0), tiles):
                    own_tile(k, i)
            sent()
            begin(late)

    for part in range(2 * T):
        r_rows(part, 2 * NC - 1, 0).wait_send()


def finish(part, held_in, acc, lta, rhs, held_ref, wg_ref, grad, sem):
    N = acc.shape[1]
    nw = pick(N, (256, 128))
    tiles = N // nw
    held = pltpu.make_async_copy(held_in, held_ref, sem.at[tiles])
    held.start()

    def tile_copy(i):
        cols = pl.ds(i * nw, nw)
        return pltpu.make_async_copy(grad.at[:, cols], wg_ref.at[0, :, cols], sem.at[i])

    for i in range(tiles):
        cols = pl.ds(i * nw, nw)
        grad[:, cols] = acc[:, cols] + jnp.dot(lta[part], rhs[part, :, cols], preferred_element_type=f32)
        tile_copy(i).start()
    for i in range(tiles):
        tile_copy(i).wait()
    held.wait()


def solution(mesh):
    S, FS, TP = mesh.shape["section"], mesh.shape["fsdp"], mesh.shape["tp"]

    def per_device(stash, grad_now, grad_top, order, gain, weight):
        MB, n, D = stash.shape[1:]
        T = grad_top.shape[0]
        wl, N = weight.shape[1:]
        NC = FS // 2
        CH = D // pick(D, (256, 128))
        WCH = len(w_cuts(wl)) - 1
        K = 2 * NC - 1
        DMA = pltpu.SemaphoreType.DMA
        V = pltpu.VMEM
        any_ = pl.BlockSpec(memory_space=pl.ANY)
        vmem = pl.BlockSpec(memory_space=V)
        peers = max(TP - 1, 1)
        outs = pl.pallas_call(
            functools.partial(kernel, S, FS, TP, T),
            out_shape=(
                V((1, n, D), bf16),
                V((wl, N), f32),
                V((2 * T, wl, FS * n), bf16),
                V((2 * T, FS * n, N), bf16),
            ),
            in_specs=[
                any_, any_, any_, any_, any_, any_,
            ],
            out_specs=(vmem,) * 4,
            scratch_shapes=[
                pltpu.SMEM((1, MB), jnp.int32),
                V((1, D), f32),
                V((FS * wl, N), bf16),
                V((MB, n, D), bf16),
                V(((T + 1) * n, D), bf16),
                V((T, n, D), bf16),
                V((T, n, 128), f32),
                V((T, n, D), bf16),
                V((2 * T, D, n), bf16),
                V(((T + 1) * n, N), f32),
                V((T, n, N), f32),
                V((T, n, D), bf16),
                V((T, peers, n, D), bf16),
                V((T, n, D), bf16),
                V((T, n, D), bf16),
                DMA((5,)), DMA((T,)),
                DMA((1,)), DMA((1 + (K - 1) * WCH,)),
                DMA((2 * T,)), DMA((2 * T, 2)),
                DMA((2 * T,)), DMA((2 * T, NC)),
                DMA((T, CH)), DMA((T, peers, CH)), DMA((T, CH)),
                DMA((2 * T,)), DMA((2 * T,)),
            ],
            compiler_params=pltpu.CompilerParams(
                collective_id=0, has_side_effects=True, vmem_limit_bytes=44 * 1024 * 1024
            ),
        )(*[pltpu.with_memory_space_constraint(o, pltpu.HBM) for o in (order, gain, stash, grad_now, grad_top, weight)])
        return pl.pallas_call(
            functools.partial(finish, 2 * T - 1),
            out_shape=(
                jax.ShapeDtypeStruct((1, n, D), bf16),
                jax.ShapeDtypeStruct((1, wl, N), f32),
            ),
            in_specs=[vmem] * 4,
            out_specs=(any_, any_),
            scratch_shapes=[V((wl, N), f32), DMA((N // pick(N, (256, 128)) + 1,))],
            compiler_params=pltpu.CompilerParams(vmem_limit_bytes=8 * 1024 * 1024),
        )(*[pltpu.with_memory_space_constraint(o, V) for o in outs])

    return jax.shard_map(
        per_device,
        mesh=mesh,
        in_specs=(
            P("section", None, "fsdp", None),
            P("section", "fsdp", None),
            P(None, "fsdp", None),
            P("section", None),
            P("section", None),
            P("section", "fsdp", "tp"),
        ),
        out_specs=(P("section", "fsdp", None), P("section", "fsdp", "tp")),
        check_vma=False,
    )
```

```python
import functools
import math

import jax
import jax.numpy as jnp
from jax import lax
from jax.experimental import pallas as pl
from jax.experimental.pallas import tpu as pltpu
from jax.sharding import PartitionSpec as P

norm_eps = 1e-06
MESH = pl.DeviceIdType.MESH
f32 = jnp.float32
bf16 = jnp.bfloat16
LAG = 4


def gelu_parts(u):
    k = 0.7978845608028654
    c = 0.044715
    u2 = u * u
    t = jnp.tanh(k * u * (1.0 + c * u2))
    half = 0.5 * (1.0 + t)
    act = u * half
    slope = half + 0.5 * u * (1.0 - t * t) * (k * (1.0 + 3.0 * c * u2))
    return act, slope


def pick(extent, options):
    for o in options:
        if extent % o == 0:
            return o
    return extent


def w_cuts(wl):
    if wl % 64 or wl <= 128:
        return (0, wl)
    deep = wl // 128 * 128
    cuts = list(range(0, deep, 256)) + [deep]
    return tuple(cuts) if deep == wl else tuple(cuts) + (wl,)


def row_step(wl):
    return math.gcd(wl, 64)


def kernel(
    S, FS, TP, T, order_in, gain_in, stash_ref, gnow_ref, gtop_ref, w_ref,
    held_ref, acc, lta, rhs,
    order_ref, gain_ref, wfull, stash, act, xt, inv, dyn, lt, prod, slope, own_e, peer_e, dxs, zin,
    lsem, topsem, w_s, w_r, l_s, l_r, r_s, r_r, e_s, e_r, z_r, x_s, x_r,
):
    s = lax.axis_index("section")
    f = lax.axis_index("fsdp")
    p = lax.axis_index("tp")
    NC = FS // 2
    SPLIT = (0, 1, 2)
    yc = f // 2
    core = f % 2
    sib = 2 * yc + (1 - core)
    n, D = act.shape[0] // (T + 1), act.shape[1]
    wl, N = w_ref.shape[1], w_ref.shape[2]
    cuts = w_cuts(wl)
    WCH = len(cuts) - 1
    wq = wl // TP
    CW = D // e_s.shape[-1]
    CH = D // CW
    nw = pick(N, (256, 128))
    tiles = N // nw
    here = CH * s // S
    there = CH * (s + 1) // S
    free = jnp.maximum(here, CH - there)

    loads = [
        pltpu.make_async_copy(w_ref.at[0], wfull.at[pl.ds(f * wl, wl), :], lsem.at[0]),
        pltpu.make_async_copy(stash_ref.at[0], stash, lsem.at[1]),
        pltpu.make_async_copy(gnow_ref.at[0], act.at[pl.ds(T * n, n), :], lsem.at[2]),
        pltpu.make_async_copy(order_in, order_ref, lsem.at[3]),
        pltpu.make_async_copy(gain_in, gain_ref, lsem.at[4]),
    ]
    for c in loads:
        c.start()

    bar = pltpu.get_barrier_semaphore()
    for r in range(1, FS):
        pl.semaphore_signal(bar, inc=1, device_id={"fsdp": (f + r) % FS}, device_id_type=MESH)
    for r in range(1, TP):
        pl.semaphore_signal(bar, inc=1, device_id={"tp": (p + r) % TP}, device_id_type=MESH)

    @pl.when(s > 0)
    def _():
        pl.semaphore_signal(bar, inc=1, device_id={"section": s - 1}, device_id_type=MESH)

    @pl.when(s < S - 1)
    def _():
        pl.semaphore_signal(bar, inc=1, device_id={"section": s + 1}, device_id_type=MESH)

    pl.semaphore_wait(bar, FS - 1 + TP - 1 + jnp.minimum(s, 1) + jnp.minimum(S - 1 - s, 1))

    def rcopy(src, dst, ss, rs, dev):
        return pltpu.make_async_remote_copy(
            src_ref=src, dst_ref=dst, send_sem=ss, recv_sem=rs, device_id=dev, device_id_type=MESH
        )

    def w_copy(k, j):
        lo, hi = cuts[j], cuts[j + 1]
        at = pl.multiple_of(lo + core * (wl - hi - lo), row_step(wl))
        if k < NC:
            rows = pl.ds(pl.multiple_of(f * wl + at, row_step(wl)), hi - lo)
            to = 2 * ((yc + k) % NC) + core
        else:
            o = k - NC + 1
            rows = pl.ds(pl.multiple_of((2 * ((yc - o + NC) % NC) + core) * wl + at, row_step(wl)), hi - lo)
            to = sib
        blk = wfull.at[rows, :]
        return rcopy(blk, blk, w_s.at[0], w_r.at[1 + (k - 1) * WCH + j], {"fsdp": to})

    def w_sib():
        blk = wfull.at[pl.ds(pl.multiple_of(f * wl, row_step(wl)), wl), :]
        return rcopy(blk, blk, w_s.at[0], w_r.at[0], {"fsdp": sib})

    loads[0].wait()
    for k in range(1, NC):
        for j in range(WCH):
            w_copy(k, j).start()
    w_sib().start()

    def is_split(part):
        return part in SPLIT and TP > 1

    def l_copy(part, k):
        cols = pl.ds(pl.multiple_of(f * n, n), n)
        if k == 0:
            to = sib
        else:
            o, cc = (k + 1) // 2, (k - 1) % 2
            to = 2 * ((yc + o) % NC) + (core + cc) % 2
        if k > 0 and is_split(part):
            src = lt.at[part, pl.ds(to * wl + p * wq, wq), :]
            dst = lta.at[part, pl.ds(p * wq, wq), cols]
        else:
            src = lt.at[part, pl.ds(to * wl, wl), :]
            dst = lta.at[part, :, cols]
        return rcopy(src, dst, l_s.at[part], l_r.at[part, min(k, 1)], {"fsdp": to})

    def x_copy(part, k, q):
        o, cc = (k + 1) // 2, (k - 1) % 2
        src_f = 2 * ((yc - o + NC) % NC) + (core + cc) % 2
        blk = lta.at[part, pl.ds(p * wq, wq), pl.ds(pl.multiple_of(src_f * n, n), n)]
        return rcopy(blk, blk, x_s.at[part], x_r.at[part], {"tp": (p + q) % TP})

    passed = set()

    def l_pass(part):
        if part in passed or not is_split(part):
            return
        passed.add(part)
        l_forward(part)

    def l_forward(part):
        l_far(part).wait_recv()
        for k in range(1, FS - 1):
            for q in range(1, TP):
                x_copy(part, k, q).start()

    def rows_of(part, rows, ss, rs):
        blk = lt.at[part, pl.ds(0, rows), :]
        return rcopy(blk, blk, ss, rs, {"fsdp": sib})

    def l_far(part):
        return rows_of(part, (FS - 2) * (wq if is_split(part) else wl), l_s.at[part], l_r.at[part, 1])

    def l_sent(part):
        return rows_of(part, wl + (FS - 2) * (wq if is_split(part) else wl), l_s.at[part], l_r.at[part, 1])

    def x_all(part):
        return rows_of(part, (FS - 2) * (TP - 1) * wq, x_s.at[part], x_r.at[part])

    def r_rows(part, count, which):
        blk = rhs.at[part, pl.ds(0, count * n), :]
        return rcopy(blk, blk, r_s.at[part], r_r.at[part, which], {"fsdp": sib})

    def l_send(part):
        for k in list(range(1, FS - 1)) + [0]:
            l_copy(part, k).start()
        lta[part, :, pl.ds(pl.multiple_of(f * n, n), n)] = lt[part, pl.ds(pl.multiple_of(f * wl, row_step(wl)), wl), :]

    def r_copy(part, k):
        if k < NC:
            at = f
            to = sib if k == 0 else 2 * ((yc + k) % NC) + core
        else:
            o = k - NC + 1
            at = 2 * ((yc - o + NC) % NC) + core
            to = sib
        blk = rhs.at[part, pl.ds(pl.multiple_of(at * n, n), n), :]
        return rcopy(blk, blk, r_s.at[part], r_r.at[part, k if 0 < k < NC else 0], {"fsdp": to})

    def r_send(part):
        for k in list(range(1, NC)) + [0]:
            r_copy(part, k).start()

    tw = pick(D, (256, 128))

    def transpose_rows(part, ref, first):
        @pl.loop(0, D // tw)
        def _(i):
            cols = pl.ds(pl.multiple_of(i * tw, tw), tw)
            lt[part, cols, :] = ref[pl.ds(first, n), cols].astype(f32).T.astype(bf16)

    loads[3].wait()
    loads[4].wait()
    loads[1].wait()
    rb = pick(n, (32, 16))
    for t in range(T):
        slot = order_ref[0, t]

        @pl.loop(0, n // rb)
        def _(i):
            rows = pl.ds(pl.multiple_of(i * rb, rb), rb)
            raw = stash[slot, rows, :]
            v = raw.astype(f32)
            iv = lax.rsqrt(jnp.mean(v * v, axis=-1, keepdims=True) + norm_eps)
            xt[t, rows, :] = raw
            inv[t, rows, :] = jnp.broadcast_to(iv, (rb, 128))
            act[pl.ds(pl.multiple_of(t * n + i * rb, rb), rb), :] = ((v * iv) * gain_ref[0:1, :]).astype(bf16)

        transpose_rows(2 * t, act, t * n)
        if t == 0:
            l_send(0)
            loads[2].wait()
            transpose_rows(1, act, T * n)
            l_send(1)
        else:
            l_send(2 * t)

    @pl.when(s == S - 1)
    def _():
        for t in range(T):
            pltpu.make_async_copy(gtop_ref.at[t], zin.at[t], topsem.at[t]).start()

    half = 2 * wl

    def part_product(chip, spans, first, width):
        @pl.loop(0, N // width)
        def _(i):
            cols = pl.ds(pl.multiple_of(i * width, width), width)
            d = None
            for lo, hi in spans:
                ks = pl.ds(pl.multiple_of(chip * half + lo, math.gcd(half, lo)), hi - lo)
                one = jnp.dot(act[:, ks], wfull[ks, cols], preferred_element_type=f32)
                d = one if d is None else d + one
            if first:
                prod[:, cols] = d
            else:
                prod[:, cols] += d

    w_sib().wait_recv()
    part_product(yc, [(0, half)], True, nw)
    for o in range(1, NC):
        for j in range(WCH):
            w_copy(o, j).wait_recv()
            w_copy(NC - 1 + o, j).start()
            w_copy(NC - 1 + o, j).wait_recv()
            lo, hi = cuts[j], cuts[j + 1]
            spans = [(lo, half - lo)] if hi == wl else [(lo, hi), (half - hi, half - lo)]
            part_product((yc - o + NC) % NC, spans, False, N if hi == wl and 0 < lo else nw)

    mine = pl.multiple_of(f * n, n)

    def gelu_rows(t, with_grad):
        @pl.loop(0, n // rb)
        def _(i):
            rows = pl.ds(pl.multiple_of(t * n + i * rb, rb), rb)
            home = pl.ds(pl.multiple_of(mine + i * rb, rb), rb)
            a, sl = gelu_parts(prod[rows, :])
            rhs[2 * t + 1, home, :] = a.astype(bf16)
            if with_grad:
                g = prod[pl.ds(pl.multiple_of(T * n + i * rb, rb), rb), :]
                rhs[2 * t, home, :] = (sl * g).astype(bf16)
            else:
                slope[t, pl.ds(pl.multiple_of(i * rb, rb), rb), :] = sl

    def e_copy(t, r, c):
        cols = pl.ds(pl.multiple_of(c * CW, CW), CW)
        return rcopy(
            own_e.at[t, :, cols], peer_e.at[t, r - 1, :, cols],
            e_s.at[t, c], e_r.at[t, r - 1, c], {"tp": (p + r) % TP},
        )

    def f_copy(t, r, c):
        cols = pl.ds(pl.multiple_of(c * CW, CW), CW)
        return rcopy(
            zin.at[t, :, cols], peer_e.at[t, r - 1, :, cols],
            e_s.at[t, c], e_r.at[t, r - 1, c], {"tp": (p + r) % TP},
        )

    def z_copy(t, c, src):
        cols = pl.ds(pl.multiple_of(c * CW, CW), CW)
        to = jnp.maximum(s - 1, 0)
        return rcopy(
            src.at[t, :, cols], zin.at[t, :, cols], e_s.at[t, c], z_r.at[t, c], {"section": to}
        )

    def held_dy(t, cols):
        return (act[pl.ds(T * n, n), cols] if t == 0 else dyn[t - 1, :, cols]).astype(f32)

    def spread(t):
        du = rhs[2 * t, pl.ds(mine, n), :]
        u = prod[pl.ds(t * n, n), :]
        m = jnp.sum(du.astype(f32) * u, axis=-1, keepdims=True) / D
        iv = inv[t, :, 0:1]
        q_scale = iv * iv * m

        @pl.loop(0, CH)
        def _(i):
            both = jnp.minimum(here, CH - here)
            far_turn = jnp.where(i < 2 * both, i % 2 == 0, CH - here > here)
            turn = jnp.where(i < 2 * both, i // 2, i - both)
            c = jnp.where(far_turn, CH - 1 - turn, here - 1 - turn)
            cols = pl.ds(pl.multiple_of(c * CW, CW), CW)
            dh = lax.dot_general(
                rhs[2 * t, pl.ds(mine, n), :], wfull[cols, :], (((1,), (1,)), ((), ())),
                preferred_element_type=f32,
            )
            e = iv * (gain_ref[0:1, cols] * dh) - xt[t, :, cols].astype(f32) * q_scale
            own_e[t, :, cols] = jnp.where((c >= here) & (p == 0), e + held_dy(t, cols), e).astype(bf16)

            @pl.when(c >= here)
            def _():
                z_copy(t, c, own_e).start()

            @pl.when(c < here)
            def _():
                for r in range(1, TP):
                    e_copy(t, r, c).start()

    def combine(t, c):
        cols = pl.ds(pl.multiple_of(c * CW, CW), CW)
        for r in range(1, TP):
            e_copy(t, r, c).wait_recv()
        total = own_e[t, :, cols].astype(f32)
        for r in range(1, TP):
            total = total + peer_e[t, r - 1, :, cols].astype(f32)
        dxs[t, :, cols] = (held_dy(t, cols) + total).astype(bf16)
        z_copy(t, c, dxs).start()

    def forward(t, c):
        z_copy(t, c, dxs).wait_recv()
        for r in range(1, TP):
            f_copy(t, r, c).start()

    def put(t, cols, value):
        if t == T - 1:
            held_ref[0, :, cols] = value
        else:
            dyn[t, :, cols] = value

    def arrive(t, c):
        cols = pl.ds(pl.multiple_of(c * CW, CW), CW)

        @pl.when((c < there) & (s < S - 1))
        def _():
            z_copy(t, c, dxs).wait_recv()

        @pl.when(c < there)
        def _():
            put(t, cols, zin[t, :, cols])

        @pl.when(c >= there)
        def _():
            total = zin[t, :, cols].astype(f32)
            for r in range(1, TP):
                f_copy(t, r, c).wait_recv()
                total = total + peer_e[t, r - 1, :, cols].astype(f32)
            put(t, cols, total.astype(bf16))

        return cols

    def relay_loop(t, consume, service):
        @pl.loop(0, CH + LAG)
        def _(i):
            @pl.when(i < CH - there)
            def _():
                forward(t, CH - 1 - i)

            @pl.when(i < here)
            def _():
                combine(t, here - 1 - i)

            service(i)

            @pl.when(i >= LAG)
            def _():
                j = i - LAG
                consume(j, CH - 1 - j)

    def at_step(i, step, fn):
        @pl.when(i == step)
        def _():
            fn()

    relayed = set()

    def r_relay(part):
        if part in relayed:
            return
        relayed.add(part)
        for o in range(1, NC):
            r_copy(part, o).wait_recv()
            r_copy(part, NC - 1 + o).start()

    parts = []
    for t in range(T):
        parts += [2 * t, 2 * t + 1]

    def own_wait(part):
        l_copy(part, 0).wait_recv()
        if is_split(part):
            x_all(part).wait_recv()
        elif FS > 2:
            l_far(part).wait_recv()
        r_rows(part, NC, 0).wait_recv()

    def own_tile(at, i):
        part = parts[at]
        cols = pl.ds(pl.multiple_of(i * nw, nw), nw)
        d = jnp.dot(lta[part], rhs[part, :, cols], preferred_element_type=f32)
        if at > 0:
            d = acc[:, cols] + d
        acc[:, cols] = d

    def sent():
        w_rows = wfull.at[pl.ds(0, (2 * NC - 1) * wl), :]
        rcopy(w_rows, w_rows, w_s.at[0], w_r.at[0], {"fsdp": sib}).wait_send()
        for part in range(2 * T):
            l_sent(part).wait_send()
            if is_split(part) and FS > 2:
                x_all(part).wait_send()
        for t in range(T):
            @pl.loop(0, CH)
            def _(c):
                crossed = (c < here) | (c >= there)

                @pl.when(crossed & (s > 0))
                def _():
                    chunk_sent(t, c, TP)

                @pl.when(crossed & (s == 0))
                def _():
                    chunk_sent(t, c, TP - 1)

                @pl.when(jnp.logical_not(crossed) & (s > 0))
                def _():
                    chunk_sent(t, c, 1)

    def chunk_sent(t, c, count):
        blk = own_e.at[t, :, pl.ds(0, count * CW)]
        if count > 0:
            rcopy(blk, blk, e_s.at[t, c], z_r.at[t, c], {"fsdp": sib}).wait_send()

    for t in range(T):
        last = t == T - 1
        if t == 0:
            gelu_rows(0, True)
            r_send(0)
            r_send(1)
        else:
            r_send(2 * t)
            l_send(2 * t + 1)

        @pl.when(s > 0)
        def _():
            spread(t)

        if t == 0:
            for later in range(1, T):
                gelu_rows(later, False)
                r_send(2 * later + 1)

        @pl.when(s == S - 1)
        def _():
            pltpu.make_async_copy(gtop_ref.at[t], zin.at[t], topsem.at[t]).wait()

        if not last:
            gr = pl.ds(T * n, n)

            def consume(j, c):
                cols = arrive(t, c)
                d = dyn[t, :, cols]
                lt[2 * t + 3, cols, :] = d.astype(f32).T.astype(bf16)
                g = jnp.dot(d, wfull[cols, :], preferred_element_type=f32)

                @pl.when(j == 0)
                def _():
                    prod[gr, :] = g

                @pl.when(j > 0)
                def _():
                    prod[gr, :] += g

            def service(i):
                if t == 0:
                    if is_split(0):
                        passed.add(0)
                        at_step(i, jnp.where(s == 0, -1, free), lambda: l_forward(0))
                    at_step(i, free, lambda: l_pass(1))
                    at_step(i, CH + LAG - 1, lambda: r_relay(0))
                    if is_split(2):
                        at_step(i, jnp.where(s == 0, CH + LAG - 1, -1), lambda: l_forward(2))

            if t == 0 and is_split(0):
                @pl.when(s == 0)
                def _():
                    l_forward(0)

            relay_loop(t, consume, service)

            @pl.loop(0, n // rb)
            def _(i):
                rows = pl.ds(pl.multiple_of(i * rb, rb), rb)
                g = prod[pl.ds(pl.multiple_of(T * n + i * rb, rb), rb), :]
                here_rows = pl.ds(pl.multiple_of(mine + i * rb, rb), rb)
                rhs[2 * t + 2, here_rows, :] = (slope[t + 1, rows, :] * g).astype(bf16)
        else:
            late = len(parts) - 1
            steps = CH + LAG

            def consume(j, c):
                arrive(t, c)

            def begin(at):
                part = parts[at]
                l_pass(part)
                r_relay(part)
                own_wait(part)

            def service(i):
                if late > 2:
                    at_step(i, 0, lambda: r_relay(parts[1]))
                    if is_split(2):
                        passed.add(2)
                        at_step(i, jnp.where(s == 0, -1, free), lambda: l_forward(2))
                    at_step(i, CH - 1, lambda: (r_relay(parts[late]), r_relay(parts[2])))
                for k in range(late):
                    first = k * tiles + (k > 1)

                    @pl.when((i >= first) & (i < first + tiles))
                    def _():
                        @pl.when(i == first)
                        def _():
                            begin(k)

                        own_tile(k, i - first)

            relay_loop(t, consume, service)
            for k in range(late):
                first = k * tiles + (k > 1)
                if first >= steps:
                    begin(k)
                for i in range(max(steps - first, 0), tiles):
                    own_tile(k, i)
            sent()
            begin(late)

    for part in range(2 * T):
        r_rows(part, 2 * NC - 1, 0).wait_send()


def finish(part, held_in, acc, lta, rhs, held_ref, wg_ref, grad, sem):
    wl = acc.shape[0]
    tiles = 4
    step = wl // tiles
    held = pltpu.make_async_copy(held_in, held_ref, sem.at[tiles])
    held.start()

    def tile_copy(i):
        rows = pl.ds(i * step, step)
        return pltpu.make_async_copy(grad.at[rows, :], wg_ref.at[0, rows, :], sem.at[i])

    for i in range(tiles):
        rows = pl.ds(i * step, step)
        grad[rows, :] = acc[rows, :] + jnp.dot(lta[part, rows, :], rhs[part], preferred_element_type=f32)
        tile_copy(i).start()
    for i in range(tiles):
        tile_copy(i).wait()
    held.wait()


def solution(mesh):
    S, FS, TP = mesh.shape["section"], mesh.shape["fsdp"], mesh.shape["tp"]

    def per_device(stash, grad_now, grad_top, order, gain, weight):
        MB, n, D = stash.shape[1:]
        T = grad_top.shape[0]
        wl, N = weight.shape[1:]
        NC = FS // 2
        CH = D // pick(D, (256, 128))
        WCH = len(w_cuts(wl)) - 1
        K = 2 * NC - 1
        DMA = pltpu.SemaphoreType.DMA
        V = pltpu.VMEM
        any_ = pl.BlockSpec(memory_space=pl.ANY)
        vmem = pl.BlockSpec(memory_space=V)
        peers = max(TP - 1, 1)
        outs = pl.pallas_call(
            functools.partial(kernel, S, FS, TP, T),
            out_shape=(
                V((1, n, D), bf16),
                V((wl, N), f32),
                V((2 * T, wl, FS * n), bf16),
                V((2 * T, FS * n, N), bf16),
            ),
            in_specs=[
                any_, any_, any_, any_, any_, any_,
            ],
            out_specs=(vmem,) * 4,
            scratch_shapes=[
                pltpu.SMEM((1, MB), jnp.int32),
                V((1, D), f32),
                V((FS * wl, N), bf16),
                V((MB, n, D), bf16),
                V(((T + 1) * n, D), bf16),
                V((T, n, D), bf16),
                V((T, n, 128), f32),
                V((T, n, D), bf16),
                V((2 * T, D, n), bf16),
                V(((T + 1) * n, N), f32),
                V((T, n, N), f32),
                V((T, n, D), bf16),
                V((T, peers, n, D), bf16),
                V((T, n, D), bf16),
                V((T, n, D), bf16),
                DMA((5,)), DMA((T,)),
                DMA((1,)), DMA((1 + (K - 1) * WCH,)),
                DMA((2 * T,)), DMA((2 * T, 2)),
                DMA((2 * T,)), DMA((2 * T, NC)),
                DMA((T, CH)), DMA((T, peers, CH)), DMA((T, CH)),
                DMA((2 * T,)), DMA((2 * T,)),
            ],
            compiler_params=pltpu.CompilerParams(
                collective_id=0, has_side_effects=True, vmem_limit_bytes=44 * 1024 * 1024
            ),
        )(*[pltpu.with_memory_space_constraint(o, pltpu.HBM) for o in (order, gain, stash, grad_now, grad_top, weight)])
        return pl.pallas_call(
            functools.partial(finish, 2 * T - 1),
            out_shape=(
                jax.ShapeDtypeStruct((1, n, D), bf16),
                jax.ShapeDtypeStruct((1, wl, N), f32),
            ),
            in_specs=[vmem] * 4,
            out_specs=(any_, any_),
            scratch_shapes=[V((wl, N), f32), DMA((9,))],
            compiler_params=pltpu.CompilerParams(vmem_limit_bytes=8 * 1024 * 1024),
        )(*[pltpu.with_memory_space_constraint(o, V) for o in outs])

    return jax.shard_map(
        per_device,
        mesh=mesh,
        in_specs=(
            P("section", None, "fsdp", None),
            P("section", "fsdp", None),
            P(None, "fsdp", None),
            P("section", None),
            P("section", None),
            P("section", "fsdp", "tp"),
        ),
        out_specs=(P("section", "fsdp", None), P("section", "fsdp", "tp")),
        check_vma=False,
    )
```

```python
import functools
import math

import jax
import jax.numpy as jnp
from jax import lax
from jax.experimental import pallas as pl
from jax.experimental.pallas import tpu as pltpu
from jax.sharding import PartitionSpec as P

norm_eps = 1e-06
MESH = pl.DeviceIdType.MESH
f32 = jnp.float32
bf16 = jnp.bfloat16
LAG = 4


def gelu_parts(u):
    k = 0.7978845608028654
    c = 0.044715
    u2 = u * u
    t = jnp.tanh(k * u * (1.0 + c * u2))
    half = 0.5 * (1.0 + t)
    act = u * half
    slope = half + 0.5 * u * (1.0 - t * t) * (k * (1.0 + 3.0 * c * u2))
    return act, slope


def pick(extent, options):
    for o in options:
        if extent % o == 0:
            return o
    return extent


def w_cuts(wl):
    if wl % 64 or wl <= 128:
        return (0, wl)
    deep = wl // 128 * 128
    cuts = list(range(0, deep, 256)) + [deep]
    return tuple(cuts) if deep == wl else tuple(cuts) + (wl,)


def row_step(wl):
    return math.gcd(wl, 64)


def kernel(
    S, FS, TP, T, order_in, gain_in, stash_ref, gnow_ref, gtop_ref, w_ref,
    held_ref, acc, lta, rhs,
    order_ref, gain_ref, wfull, stash, act, xt, inv, dyn, lt, prod, slope, own_e, peer_e, dxs, zin,
    lsem, topsem, w_s, w_r, l_s, l_r, r_s, r_r, e_s, e_r, z_r, x_s, x_r,
):
    s = lax.axis_index("section")
    f = lax.axis_index("fsdp")
    p = lax.axis_index("tp")
    NC = FS // 2
    SPLIT = (0, 1, 2)
    yc = f // 2
    core = f % 2
    sib = 2 * yc + (1 - core)
    n, D = act.shape[0] // (T + 1), act.shape[1]
    wl, N = w_ref.shape[1], w_ref.shape[2]
    cuts = w_cuts(wl)
    WCH = len(cuts) - 1
    wq = wl // TP
    CW = D // e_s.shape[-1]
    CH = D // CW
    nw = pick(N, (256, 128))
    tiles = N // nw
    here = CH * s // S
    there = CH * (s + 1) // S
    free = jnp.maximum(here, CH - there)

    loads = [
        pltpu.make_async_copy(w_ref.at[0], wfull.at[pl.ds(f * wl, wl), :], lsem.at[0]),
        pltpu.make_async_copy(stash_ref.at[0], stash, lsem.at[1]),
        pltpu.make_async_copy(gnow_ref.at[0], act.at[pl.ds(T * n, n), :], lsem.at[2]),
        pltpu.make_async_copy(order_in, order_ref, lsem.at[3]),
        pltpu.make_async_copy(gain_in, gain_ref, lsem.at[4]),
    ]
    bar = pltpu.get_barrier_semaphore()
    for r in range(1, FS):
        pl.semaphore_signal(bar, inc=1, device_id={"fsdp": (f + r) % FS}, device_id_type=MESH)
    for r in range(1, TP):
        pl.semaphore_signal(bar, inc=1, device_id={"tp": (p + r) % TP}, device_id_type=MESH)

    @pl.when(s > 0)
    def _():
        pl.semaphore_signal(bar, inc=1, device_id={"section": s - 1}, device_id_type=MESH)

    @pl.when(s < S - 1)
    def _():
        pl.semaphore_signal(bar, inc=1, device_id={"section": s + 1}, device_id_type=MESH)

    for c in loads:
        c.start()

    pl.semaphore_wait(bar, FS - 1 + TP - 1 + jnp.minimum(s, 1) + jnp.minimum(S - 1 - s, 1))

    def rcopy(src, dst, ss, rs, dev):
        return pltpu.make_async_remote_copy(
            src_ref=src, dst_ref=dst, send_sem=ss, recv_sem=rs, device_id=dev, device_id_type=MESH
        )

    def w_copy(k, j):
        lo, hi = cuts[j], cuts[j + 1]
        at = pl.multiple_of(lo + core * (wl - hi - lo), row_step(wl))
        if k < NC:
            rows = pl.ds(pl.multiple_of(f * wl + at, row_step(wl)), hi - lo)
            to = 2 * ((yc + k) % NC) + core
        else:
            o = k - NC + 1
            rows = pl.ds(pl.multiple_of((2 * ((yc - o + NC) % NC) + core) * wl + at, row_step(wl)), hi - lo)
            to = sib
        blk = wfull.at[rows, :]
        return rcopy(blk, blk, w_s.at[0], w_r.at[1 + (k - 1) * WCH + j], {"fsdp": to})

    def w_sib():
        blk = wfull.at[pl.ds(pl.multiple_of(f * wl, row_step(wl)), wl), :]
        return rcopy(blk, blk, w_s.at[0], w_r.at[0], {"fsdp": sib})

    loads[0].wait()
    for k in range(1, NC):
        for j in range(WCH):
            w_copy(k, j).start()
    w_sib().start()

    def is_split(part):
        return part in SPLIT and TP > 1

    def l_copy(part, k):
        cols = pl.ds(pl.multiple_of(f * n, n), n)
        if k == 0:
            to = sib
        else:
            o, cc = (k + 1) // 2, (k - 1) % 2
            to = 2 * ((yc + o) % NC) + (core + cc) % 2
        if k > 0 and is_split(part):
            src = lt.at[part, pl.ds(to * wl + p * wq, wq), :]
            dst = lta.at[part, pl.ds(p * wq, wq), cols]
        else:
            src = lt.at[part, pl.ds(to * wl, wl), :]
            dst = lta.at[part, :, cols]
        return rcopy(src, dst, l_s.at[part], l_r.at[part, min(k, 1)], {"fsdp": to})

    def x_copy(part, k, q):
        o, cc = (k + 1) // 2, (k - 1) % 2
        src_f = 2 * ((yc - o + NC) % NC) + (core + cc) % 2
        blk = lta.at[part, pl.ds(p * wq, wq), pl.ds(pl.multiple_of(src_f * n, n), n)]
        return rcopy(blk, blk, x_s.at[part], x_r.at[part], {"tp": (p + q) % TP})

    passed = set()

    def l_pass(part):
        if part in passed or not is_split(part):
            return
        passed.add(part)
        l_forward(part)

    def l_forward(part):
        l_far(part).wait_recv()
        for k in range(1, FS - 1):
            for q in range(1, TP):
                x_copy(part, k, q).start()

    def rows_of(part, rows, ss, rs):
        blk = lt.at[part, pl.ds(0, rows), :]
        return rcopy(blk, blk, ss, rs, {"fsdp": sib})

    def l_far(part):
        return rows_of(part, (FS - 2) * (wq if is_split(part) else wl), l_s.at[part], l_r.at[part, 1])

    def l_sent(part):
        return rows_of(part, wl + (FS - 2) * (wq if is_split(part) else wl), l_s.at[part], l_r.at[part, 1])

    def x_all(part):
        return rows_of(part, (FS - 2) * (TP - 1) * wq, x_s.at[part], x_r.at[part])

    def r_rows(part, count, which):
        blk = rhs.at[part, pl.ds(0, count * n), :]
        return rcopy(blk, blk, r_s.at[part], r_r.at[part, which], {"fsdp": sib})

    def l_send(part):
        for k in list(range(1, FS - 1)) + [0]:
            l_copy(part, k).start()
        lta[part, :, pl.ds(pl.multiple_of(f * n, n), n)] = lt[part, pl.ds(pl.multiple_of(f * wl, row_step(wl)), wl), :]

    def r_copy(part, k):
        if k < NC:
            at = f
            to = sib if k == 0 else 2 * ((yc + k) % NC) + core
        else:
            o = k - NC + 1
            at = 2 * ((yc - o + NC) % NC) + core
            to = sib
        blk = rhs.at[part, pl.ds(pl.multiple_of(at * n, n), n), :]
        return rcopy(blk, blk, r_s.at[part], r_r.at[part, min(k, NC)], {"fsdp": to})

    def r_send(part):
        for k in list(range(1, NC)) + [0]:
            r_copy(part, k).start()

    tw = pick(D, (256, 128))

    def transpose_rows(part, ref, first):
        @pl.loop(0, D // tw)
        def _(i):
            cols = pl.ds(pl.multiple_of(i * tw, tw), tw)
            lt[part, cols, :] = ref[pl.ds(first, n), cols].astype(f32).T.astype(bf16)

    loads[3].wait()
    loads[4].wait()
    loads[1].wait()
    rb = pick(n, (32, 16))
    for t in range(T):
        slot = order_ref[0, t]

        @pl.loop(0, n // rb)
        def _(i):
            rows = pl.ds(pl.multiple_of(i * rb, rb), rb)
            raw = stash[slot, rows, :]
            v = raw.astype(f32)
            iv = lax.rsqrt(jnp.mean(v * v, axis=-1, keepdims=True) + norm_eps)
            xt[t, rows, :] = raw
            inv[t, rows, :] = jnp.broadcast_to(iv, (rb, 128))
            act[pl.ds(pl.multiple_of(t * n + i * rb, rb), rb), :] = ((v * iv) * gain_ref[0:1, :]).astype(bf16)

        transpose_rows(2 * t, act, t * n)
        if t == 0:
            l_send(0)
            loads[2].wait()
            transpose_rows(1, act, T * n)
            l_send(1)
        else:
            l_send(2 * t)

    @pl.when(s == S - 1)
    def _():
        for t in range(T):
            pltpu.make_async_copy(gtop_ref.at[t], zin.at[t], topsem.at[t]).start()

    half = 2 * wl

    def part_product(chip, spans, first, width):
        @pl.loop(0, N // width)
        def _(i):
            cols = pl.ds(pl.multiple_of(i * width, width), width)
            d = None
            for lo, hi in spans:
                ks = pl.ds(pl.multiple_of(chip * half + lo, math.gcd(half, lo)), hi - lo)
                one = jnp.dot(act[:, ks], wfull[ks, cols], preferred_element_type=f32)
                d = one if d is None else d + one
            if first:
                prod[:, cols] = d
            else:
                prod[:, cols] += d

    w_sib().wait_recv()
    part_product(yc, [(0, half)], True, nw)
    for o in range(1, NC):
        for j in range(WCH):
            w_copy(o, j).wait_recv()
            w_copy(NC - 1 + o, j).start()
            w_copy(NC - 1 + o, j).wait_recv()
            lo, hi = cuts[j], cuts[j + 1]
            spans = [(lo, half - lo)] if hi == wl else [(lo, hi), (half - hi, half - lo)]
            part_product((yc - o + NC) % NC, spans, False, N if hi == wl and 0 < lo else nw)

    mine = pl.multiple_of(f * n, n)

    def gelu_rows(t, with_grad):
        @pl.loop(0, n // rb)
        def _(i):
            rows = pl.ds(pl.multiple_of(t * n + i * rb, rb), rb)
            home = pl.ds(pl.multiple_of(mine + i * rb, rb), rb)
            a, sl = gelu_parts(prod[rows, :])
            rhs[2 * t + 1, home, :] = a.astype(bf16)
            if with_grad:
                g = prod[pl.ds(pl.multiple_of(T * n + i * rb, rb), rb), :]
                rhs[2 * t, home, :] = (sl * g).astype(bf16)
            else:
                slope[t, pl.ds(pl.multiple_of(i * rb, rb), rb), :] = sl

    def e_copy(t, r, c):
        cols = pl.ds(pl.multiple_of(c * CW, CW), CW)
        return rcopy(
            own_e.at[t, :, cols], peer_e.at[t, r - 1, :, cols],
            e_s.at[t, c], e_r.at[t, r - 1, c], {"tp": (p + r) % TP},
        )

    def f_copy(t, r, c):
        cols = pl.ds(pl.multiple_of(c * CW, CW), CW)
        return rcopy(
            zin.at[t, :, cols], peer_e.at[t, r - 1, :, cols],
            e_s.at[t, c], e_r.at[t, r - 1, c], {"tp": (p + r) % TP},
        )

    def z_copy(t, c, src):
        cols = pl.ds(pl.multiple_of(c * CW, CW), CW)
        to = jnp.maximum(s - 1, 0)
        return rcopy(
            src.at[t, :, cols], zin.at[t, :, cols], e_s.at[t, c], z_r.at[t, c], {"section": to}
        )

    def held_dy(t, cols):
        return (act[pl.ds(T * n, n), cols] if t == 0 else dyn[t - 1, :, cols]).astype(f32)

    def spread(t):
        du = rhs[2 * t, pl.ds(mine, n), :]
        u = prod[pl.ds(t * n, n), :]
        m = jnp.sum(du.astype(f32) * u, axis=-1, keepdims=True) / D
        iv = inv[t, :, 0:1]
        q_scale = iv * iv * m

        @pl.loop(0, CH)
        def _(i):
            both = jnp.minimum(here, CH - here)
            far_turn = jnp.where(i < 2 * both, i % 2 == 0, CH - here > here)
            turn = jnp.where(i < 2 * both, i // 2, i - both)
            c = jnp.where(far_turn, CH - 1 - turn, here - 1 - turn)
            cols = pl.ds(pl.multiple_of(c * CW, CW), CW)
            dh = lax.dot_general(
                rhs[2 * t, pl.ds(mine, n), :], wfull[cols, :], (((1,), (1,)), ((), ())),
                preferred_element_type=f32,
            )
            e = iv * (gain_ref[0:1, cols] * dh) - xt[t, :, cols].astype(f32) * q_scale
            own_e[t, :, cols] = jnp.where((c >= here) & (p == 0), e + held_dy(t, cols), e).astype(bf16)

            @pl.when(c >= here)
            def _():
                z_copy(t, c, own_e).start()

            @pl.when(c < here)
            def _():
                for r in range(1, TP):
                    e_copy(t, r, c).start()

    def combine(t, c):
        cols = pl.ds(pl.multiple_of(c * CW, CW), CW)
        for r in range(1, TP):
            e_copy(t, r, c).wait_recv()
        total = own_e[t, :, cols].astype(f32)
        for r in range(1, TP):
            total = total + peer_e[t, r - 1, :, cols].astype(f32)
        dxs[t, :, cols] = (held_dy(t, cols) + total).astype(bf16)
        z_copy(t, c, dxs).start()

    def forward(t, c):
        z_copy(t, c, dxs).wait_recv()
        for r in range(1, TP):
            f_copy(t, r, c).start()

    def put(t, cols, value):
        if t == T - 1:
            held_ref[0, :, cols] = value
        else:
            dyn[t, :, cols] = value

    def arrive(t, c):
        cols = pl.ds(pl.multiple_of(c * CW, CW), CW)

        @pl.when((c < there) & (s < S - 1))
        def _():
            z_copy(t, c, dxs).wait_recv()

        @pl.when(c < there)
        def _():
            put(t, cols, zin[t, :, cols])

        @pl.when(c >= there)
        def _():
            total = zin[t, :, cols].astype(f32)
            for r in range(1, TP):
                f_copy(t, r, c).wait_recv()
                total = total + peer_e[t, r - 1, :, cols].astype(f32)
            put(t, cols, total.astype(bf16))

        return cols

    def relay_loop(t, consume, service):
        @pl.loop(0, CH + LAG)
        def _(i):
            @pl.when(i < CH - there)
            def _():
                forward(t, CH - 1 - i)

            @pl.when(i < here)
            def _():
                combine(t, here - 1 - i)

            service(i)

            @pl.when(i >= LAG)
            def _():
                j = i - LAG
                consume(j, CH - 1 - j)

    def at_step(i, step, fn):
        @pl.when(i == step)
        def _():
            fn()

    relayed = set()

    def r_relay(part):
        if part in relayed:
            return
        relayed.add(part)
        for o in range(1, NC):
            r_copy(part, o).wait_recv()
            r_copy(part, NC - 1 + o).start()

    parts = []
    for t in range(T):
        parts += [2 * t, 2 * t + 1]

    def own_wait(part):
        chip_wait(part)
        far_wait(part)

    def chip_wait(part):
        l_copy(part, 0).wait_recv()
        r_copy(part, 0).wait_recv()

    def far_wait(part):
        if is_split(part):
            x_all(part).wait_recv()
        elif FS > 2:
            l_far(part).wait_recv()
        if NC > 1:
            r_rows(part, NC - 1, NC).wait_recv()

    def chip_tile(at, i, chips):
        part = parts[at]
        cols = pl.ds(pl.multiple_of(i * nw, nw), nw)
        d = acc[:, cols]
        for o in chips:
            ks = pl.ds(pl.multiple_of((yc + o) % NC * (2 * n), 2 * n), 2 * n)
            d = d + jnp.dot(lta[part, :, ks], rhs[part, ks, cols], preferred_element_type=f32)
        acc[:, cols] = d

    def own_tile(at, i):
        part = parts[at]
        cols = pl.ds(pl.multiple_of(i * nw, nw), nw)
        d = jnp.dot(lta[part], rhs[part, :, cols], preferred_element_type=f32)
        if at > 0:
            d = acc[:, cols] + d
        acc[:, cols] = d

    def sent():
        w_rows = wfull.at[pl.ds(0, (2 * NC - 1) * wl), :]
        rcopy(w_rows, w_rows, w_s.at[0], w_r.at[0], {"fsdp": sib}).wait_send()
        for part in range(2 * T):
            l_sent(part).wait_send()
            if is_split(part) and FS > 2:
                x_all(part).wait_send()
        for t in range(T):
            @pl.loop(0, CH)
            def _(c):
                crossed = (c < here) | (c >= there)

                @pl.when(crossed & (s > 0))
                def _():
                    chunk_sent(t, c, TP)

                @pl.when(crossed & (s == 0))
                def _():
                    chunk_sent(t, c, TP - 1)

                @pl.when(jnp.logical_not(crossed) & (s > 0))
                def _():
                    chunk_sent(t, c, 1)

    def chunk_sent(t, c, count):
        blk = own_e.at[t, :, pl.ds(0, count * CW)]
        if count > 0:
            rcopy(blk, blk, e_s.at[t, c], z_r.at[t, c], {"fsdp": sib}).wait_send()

    for t in range(T):
        last = t == T - 1
        if t == 0:
            gelu_rows(0, True)
            r_send(0)
            r_send(1)
        else:
            r_send(2 * t)
            l_send(2 * t + 1)

        @pl.when(s > 0)
        def _():
            spread(t)

        if t == 0:
            for later in range(1, T):
                gelu_rows(later, False)
                r_send(2 * later + 1)

        @pl.when(s == S - 1)
        def _():
            pltpu.make_async_copy(gtop_ref.at[t], zin.at[t], topsem.at[t]).wait()

        if not last:
            gr = pl.ds(T * n, n)

            def consume(j, c):
                cols = arrive(t, c)
                d = dyn[t, :, cols]
                lt[2 * t + 3, cols, :] = d.astype(f32).T.astype(bf16)
                g = jnp.dot(d, wfull[cols, :], preferred_element_type=f32)

                @pl.when(j == 0)
                def _():
                    prod[gr, :] = g

                @pl.when(j > 0)
                def _():
                    prod[gr, :] += g

            def service(i):
                if t == 0:
                    if is_split(0):
                        passed.add(0)
                        at_step(i, jnp.where(s == 0, -1, free), lambda: l_forward(0))
                    at_step(i, free, lambda: l_pass(1))
                    at_step(i, CH + LAG - 1, lambda: r_relay(0))
                    if is_split(2):
                        at_step(i, jnp.where(s == 0, CH + LAG - 1, -1), lambda: l_forward(2))

            if t == 0 and is_split(0):
                @pl.when(s == 0)
                def _():
                    l_forward(0)

            relay_loop(t, consume, service)

            @pl.loop(0, n // rb)
            def _(i):
                rows = pl.ds(pl.multiple_of(i * rb, rb), rb)
                g = prod[pl.ds(pl.multiple_of(T * n + i * rb, rb), rb), :]
                here_rows = pl.ds(pl.multiple_of(mine + i * rb, rb), rb)
                rhs[2 * t + 2, here_rows, :] = (slope[t + 1, rows, :] * g).astype(bf16)
        else:
            late = len(parts) - 1
            steps = CH + LAG
            near_at, far_at = tiles, steps - tiles
            halves = late > 1 and NC > 1 and 2 * tiles <= far_at
            whole = late - 1 if halves else late

            def consume(j, c):
                arrive(t, c)

            def begin(at):
                part = parts[at]
                l_pass(part)
                r_relay(part)
                own_wait(part)

            def service(i):
                if late > 2:
                    at_step(i, 0, lambda: r_relay(parts[1]))
                    if is_split(2):
                        passed.add(2)
                        at_step(i, jnp.where(s == 0, -1, free), lambda: l_forward(2))
                    at_step(i, CH - 1, lambda: (r_relay(parts[late]), r_relay(parts[2])))
                for k in range(whole):
                    @pl.when((i >= k * tiles) & (i < (k + 1) * tiles))
                    def _():
                        @pl.when(i == k * tiles)
                        def _():
                            begin(k)

                        own_tile(k, i - k * tiles)

                if halves:
                    k = late - 1

                    @pl.when((i >= near_at) & (i < near_at + tiles))
                    def _():
                        @pl.when(i == near_at)
                        def _():
                            chip_wait(parts[k])

                        chip_tile(k, i - near_at, [0])

                    @pl.when((i >= far_at) & (i < far_at + tiles))
                    def _():
                        @pl.when(i == far_at)
                        def _():
                            l_pass(parts[k])
                            r_relay(parts[k])
                            far_wait(parts[k])

                        chip_tile(k, i - far_at, range(1, NC))

            relay_loop(t, consume, service)
            for k in range(whole):
                if k * tiles >= steps:
                    begin(k)
                for i in range(max(steps - k * tiles, 0), tiles):
                    own_tile(k, i)
            sent()
            begin(late)

    for part in range(2 * T):
        r_rows(part, 2 * NC - 1, 0).wait_send()


def finish(part, held_in, acc, lta, rhs, held_ref, wg_ref, grad, sem):
    wl = acc.shape[0]
    tiles = 4
    step = wl // tiles
    held = pltpu.make_async_copy(held_in, held_ref, sem.at[tiles])
    held.start()

    def tile_copy(i):
        rows = pl.ds(i * step, step)
        return pltpu.make_async_copy(grad.at[rows, :], wg_ref.at[0, rows, :], sem.at[i])

    for i in range(tiles):
        rows = pl.ds(i * step, step)
        grad[rows, :] = acc[rows, :] + jnp.dot(lta[part, rows, :], rhs[part], preferred_element_type=f32)
        tile_copy(i).start()
    for i in range(tiles):
        tile_copy(i).wait()
    held.wait()


def solution(mesh):
    S, FS, TP = mesh.shape["section"], mesh.shape["fsdp"], mesh.shape["tp"]

    def per_device(stash, grad_now, grad_top, order, gain, weight):
        MB, n, D = stash.shape[1:]
        T = grad_top.shape[0]
        wl, N = weight.shape[1:]
        NC = FS // 2
        CH = D // pick(D, (256, 128))
        WCH = len(w_cuts(wl)) - 1
        K = 2 * NC - 1
        DMA = pltpu.SemaphoreType.DMA
        V = pltpu.VMEM
        any_ = pl.BlockSpec(memory_space=pl.ANY)
        vmem = pl.BlockSpec(memory_space=V)
        peers = max(TP - 1, 1)
        outs = pl.pallas_call(
            functools.partial(kernel, S, FS, TP, T),
            out_shape=(
                V((1, n, D), bf16),
                V((wl, N), f32),
                V((2 * T, wl, FS * n), bf16),
                V((2 * T, FS * n, N), bf16),
            ),
            in_specs=[
                any_, any_, any_, any_, any_, any_,
            ],
            out_specs=(vmem,) * 4,
            scratch_shapes=[
                pltpu.SMEM((1, MB), jnp.int32),
                V((1, D), f32),
                V((FS * wl, N), bf16),
                V((MB, n, D), bf16),
                V(((T + 1) * n, D), bf16),
                V((T, n, D), bf16),
                V((T, n, 128), f32),
                V((T, n, D), bf16),
                V((2 * T, D, n), bf16),
                V(((T + 1) * n, N), f32),
                V((T, n, N), f32),
                V((T, n, D), bf16),
                V((T, peers, n, D), bf16),
                V((T, n, D), bf16),
                V((T, n, D), bf16),
                DMA((5,)), DMA((T,)),
                DMA((1,)), DMA((1 + (K - 1) * WCH,)),
                DMA((2 * T,)), DMA((2 * T, 2)),
                DMA((2 * T,)), DMA((2 * T, NC + 1)),
                DMA((T, CH)), DMA((T, peers, CH)), DMA((T, CH)),
                DMA((2 * T,)), DMA((2 * T,)),
            ],
            compiler_params=pltpu.CompilerParams(
                collective_id=0, has_side_effects=True, vmem_limit_bytes=44 * 1024 * 1024
            ),
        )(*[pltpu.with_memory_space_constraint(o, pltpu.HBM) for o in (order, gain, stash, grad_now, grad_top, weight)])
        return pl.pallas_call(
            functools.partial(finish, 2 * T - 1),
            out_shape=(
                jax.ShapeDtypeStruct((1, n, D), bf16),
                jax.ShapeDtypeStruct((1, wl, N), f32),
            ),
            in_specs=[vmem] * 4,
            out_specs=(any_, any_),
            scratch_shapes=[V((wl, N), f32), DMA((9,))],
            compiler_params=pltpu.CompilerParams(vmem_limit_bytes=8 * 1024 * 1024),
        )(*[pltpu.with_memory_space_constraint(o, V) for o in outs])

    return jax.shard_map(
        per_device,
        mesh=mesh,
        in_specs=(
            P("section", None, "fsdp", None),
            P("section", "fsdp", None),
            P(None, "fsdp", None),
            P("section", None),
            P("section", None),
            P("section", "fsdp", "tp"),
        ),
        out_specs=(P("section", "fsdp", None), P("section", "fsdp", "tp")),
        check_vma=False,
    )
```
